8 devices in a mesh: data: 1 (over z), col: 2 (over y), row: 4 (over x, core).
Axes of the slice: x: 2, y: 2, z: 1, core: 2. Of those that a mesh axis runs over, the one named last changes fastest.
Arguments:
- residual: bfloat16 [128, 3072], P('data', 'row')
- gain_mlp: float32 [3072], P('row')
- gain_attn: float32 [3072], P('row')
- w_gate: bfloat16 [3072, 24576], P(None, ('col', 'row'))
- w_up: bfloat16 [3072, 24576], P(None, ('col', 'row'))
- w_down: bfloat16 [24576, 3072], P('col', 'row')
- w_qkv: bfloat16 [3072, 12288], P(None, ('col', 'row'))
Outputs:
- output 1: bfloat16 [128, 3072], P('data', 'row')
- output 2: bfloat16 [128, 12288], P('data', ('col', 'row'))
All inputs are finite; a program needn't handle non-finite values.
Results may differ from the reference program's by a relative error of at most 0.00415185.
Values are sent between devices in bfloat16 or wider.
A program may use at most 1 GiB of HBM per device.

```python
import math
import jax
import jax.numpy as jnp
from jax import lax

TOKENS = 128
D = 3072
FF = 24576
HEADS = 16
KV_HEADS = 16
HEAD_DIM = 256
QKV_WIDTH = (HEADS + 2 * KV_HEADS) * HEAD_DIM
NORM_EPS = 1e-6


def setup_inputs(seed: int = 0, part: int = 0) -> dict:
    key_list = jax.random.split(jax.random.key(seed), 8)
    tok_keys = jax.random.split(jax.random.fold_in(key_list[0], part), 3)
    base_vals = jax.random.normal(tok_keys[0], (TOKENS, D), jnp.float32)
    tok_scale = jnp.exp(jax.random.uniform(tok_keys[1], (TOKENS, 1), jnp.float32, -1.0, 1.0))
    wave_amps = jax.random.normal(tok_keys[2], (TOKENS, 2), jnp.float32)
    angles = jnp.arange(D, dtype=jnp.float32) * (2.0 * math.pi / D)
    profile = jnp.exp(0.7 * (wave_amps[:, 0:1] * jnp.cos(angles) + wave_amps[:, 1:2] * jnp.sin(angles)))
    residual = (base_vals * tok_scale * profile).astype(jnp.bfloat16)
    gain_mlp = jax.random.uniform(key_list[1], (D,), jnp.float32, 0.4, 1.6)
    gain_attn = jax.random.uniform(key_list[2], (D,), jnp.float32, 0.4, 1.6)
    w_gate = (jax.random.normal(key_list[3], (D, FF), jnp.float32) * D ** -0.5).astype(jnp.bfloat16)
    w_up = (jax.random.normal(key_list[4], (D, FF), jnp.float32) * D ** -0.5).astype(jnp.bfloat16)
    w_down = (jax.random.normal(key_list[5], (FF, D), jnp.float32) * FF ** -0.5).astype(jnp.bfloat16)
    w_qkv = (jax.random.normal(key_list[6], (D, QKV_WIDTH), jnp.float32) * D ** -0.5).astype(jnp.bfloat16)
    return {'residual': residual, 'gain_mlp': gain_mlp, 'gain_attn': gain_attn, 'w_gate': w_gate, 'w_up': w_up, 'w_down': w_down, 'w_qkv': w_qkv}


def rms_normed(rows, gain):
    rows_f = rows.astype(jnp.float32)
    row_scale = lax.rsqrt(jnp.mean(rows_f * rows_f, axis=1, keepdims=True) + NORM_EPS)
    return (rows_f * row_scale * gain).astype(jnp.bfloat16)


def reference(residual, gain_mlp, gain_attn, w_gate, w_up, w_down, w_qkv):
    normed = rms_normed(residual, gain_mlp)
    gate_val = jnp.dot(normed, w_gate, preferred_element_type=jnp.float32)
    up_val = jnp.dot(normed, w_up, preferred_element_type=jnp.float32)
    act_val = (jax.nn.silu(gate_val) * up_val).astype(jnp.bfloat16)
    down_val = jnp.dot(act_val, w_down, preferred_element_type=jnp.float32)
    resid_next = (residual.astype(jnp.float32) + down_val).astype(jnp.bfloat16)
    normed_next = rms_normed(resid_next, gain_attn)
    qkv_out = jnp.dot(normed_next, w_qkv, preferred_element_type=jnp.float32).astype(jnp.bfloat16)
    return (resid_next, qkv_out)
```

```python
import functools

import jax
import jax.numpy as jnp
from jax import lax
from jax.experimental import pallas as pl
from jax.experimental.pallas import tpu as pltpu
from jax.sharding import PartitionSpec as P

NORM_EPS = 1e-6
MESH = pl.DeviceIdType.MESH
F32 = jnp.float32
BF16 = jnp.bfloat16

CB = 256
PASSES = ((0, 64), (64, 64))
GROUPS = ((0, 64), (64, 32), (96, 32))
AHEAD = 8


def kernel(res_h, g1_h, g2_h, wg_h, wu_h, wd_h, wq_h, xo, qo,
           wgu, wdb, abuf, xbuf, xpbuf, nbuf, acc, ybuf, gbuf,
           lsem, wsem, wdsem, wqsem, xs, xr, gs, gr, as_, ar, ys, yr, ps, pr):
    row, col = lax.axis_index('row'), lax.axis_index('col')
    mate = row + 1 - 2 * lax.rem(row, 2)
    near = lax.rem(row + 2, 4)
    far = lax.rem(mate + 2, 4)
    d_ff = wg_h.shape[1]
    chunks = d_ff // CB
    hid = res_h.shape[1]
    d_model = 4 * hid
    q_slabs = wq_h.shape[1] // CB

    def remote(src, dst, send, recv, device):
        return pltpu.make_async_remote_copy(src_ref=src, dst_ref=dst, send_sem=send, recv_sem=recv,
                                            device_id=device, device_id_type=MESH)

    def push(at, send, recv, kind):
        slot = (row, row, near)[kind]
        return remote(at(slot), at(slot), send(kind), recv(kind), {'row': (near, mate, mate)[kind]})

    def arrived(at, send, recv, kind):
        slot = (near, mate, far)[kind]
        remote(at(slot), at(slot), send(kind), recv(kind), {'row': mate}).wait_recv()

    def x_ex(p):
        t0, m = PASSES[p]
        return (lambda s: xbuf.at[s, pl.ds(t0, m)]), (lambda k: xs.at[p, k]), (lambda k: xr.at[p, k])

    g_ex = (lambda s: gbuf.at[s]), (lambda k: gs.at[k]), (lambda k: gr.at[k])

    def a_ex(g, j):
        t0, m = GROUPS[g]
        return (lambda s: abuf.at[j, s, pl.ds(t0, m)]), (lambda k: as_.at[g, j, k]), (lambda k: ar.at[g, j, k])

    def p_ex(g):
        t0, m = GROUPS[g]
        return (lambda s: xpbuf.at[s, pl.ds(t0, m)]), (lambda k: ps.at[g, k]), (lambda k: pr.at[g, k])

    def y_copy(g):
        rows = pl.ds(*GROUPS[g])
        return remote(acc.at[rows], ybuf.at[rows], ys.at[g], yr.at[g], {'col': 1 - col})

    def w_copy(j, half):
        src = (wg_h, wu_h)[half]
        start = j * CB if isinstance(j, int) else pl.multiple_of(j * CB, CB)
        return pltpu.make_async_copy(src.at[:, pl.ds(start, CB)], wgu.at[j, half], wsem.at[j, half])

    def wd_copy(j, s):
        start = pl.multiple_of(s * d_ff + j * CB, CB)
        return pltpu.make_async_copy(wd_h.at[pl.ds(start, CB)], wdb.at[j, pl.ds(s * CB, CB)], wdsem.at[j, s])

    def wq_copy(j):
        return pltpu.make_async_copy(wq_h.at[:, pl.ds(pl.multiple_of(j * CB, CB), CB)], wgu.at[j, 0], wqsem.at[j])

    loads = [pltpu.make_async_copy(res_h, xbuf.at[row], lsem.at[0]),
             pltpu.make_async_copy(g1_h, gbuf.at[row, 0], lsem.at[1]),
             pltpu.make_async_copy(g2_h, gbuf.at[row, 1], lsem.at[2])]
    for copy in loads:
        copy.start()
    for j in range(AHEAD):
        w_copy(j, 0).start()
        w_copy(j, 1).start()

    barrier = pltpu.get_barrier_semaphore()
    for device in ({'row': mate}, {'row': near}, {'col': 1 - col}):
        pl.semaphore_signal(barrier, inc=1, device_id=device, device_id_type=MESH)
    pl.semaphore_wait(barrier, 3)

    for copy in loads:
        copy.wait()
    push(*x_ex(0), 0).start()
    push(*g_ex, 0).start()
    push(*x_ex(0), 1).start()
    push(*g_ex, 1).start()
    push(*x_ex(1), 0).start()
    push(*x_ex(1), 1).start()
    acc[...] = jnp.zeros_like(acc)

    def normalise(src, which, t0, m):
        step = 16
        scales = []
        for t in range(t0, t0 + m, step):
            total = jnp.zeros((step, hid), F32)
            for q in range(4):
                v = src[q, t:t + step, :].astype(F32)
                total = total + v * v
            scales.append(lax.rsqrt(jnp.sum(total, axis=1, keepdims=True) / d_model + NORM_EPS))
        for i, t in enumerate(range(t0, t0 + m, step)):
            for q in range(4):
                v = src[q, t:t + step, :].astype(F32)
                nbuf[t:t + step, q * hid:(q + 1) * hid] = (v * scales[i] * gbuf[q, which:which + 1, :]).astype(BF16)

    arrived(*g_ex, 0)
    push(*g_ex, 2).start()
    arrived(*x_ex(0), 0)
    push(*x_ex(0), 2).start()
    for kind in (1, 2):
        arrived(*g_ex, kind)
        arrived(*x_ex(0), kind)
    normalise(xbuf, 0, *PASSES[0])

    def gate_up(p, j):
        t0, m = PASSES[p]
        n = nbuf[t0:t0 + m, :]
        gate = jnp.dot(n, wgu[j, 0], preferred_element_type=F32)
        up = jnp.dot(n, wgu[j, 1], preferred_element_type=F32)
        abuf[j, row, t0:t0 + m, :] = (jax.nn.silu(gate) * up).astype(BF16)

    def relay(g, j):
        arrived(*a_ex(g, j), 0)
        push(*a_ex(g, j), 2).start()

    def down_wait(g, j, first):
        arrived(*a_ex(g, j), 1)
        arrived(*a_ex(g, j), 2)
        if first:
            for s in range(4):
                wd_copy(j, s).wait()

    def down(g, j, n=1):
        t0, m = GROUPS[g]
        a = jnp.concatenate([abuf[j + i, s, t0:t0 + m, :] for i in range(n) for s in range(4)], axis=1)
        w = wdb[pl.ds(j, n)].reshape(n * 4 * CB, hid)
        acc[t0:t0 + m, :] += jnp.dot(a, w, preferred_element_type=F32)

    def first_pass(j, carry):
        @pl.when(j + AHEAD < chunks)
        def _():
            w_copy(j + AHEAD, 0).start()
            w_copy(j + AHEAD, 1).start()

        @pl.when(j == chunks - AHEAD)
        def _():
            def issue(i, c):
                for s in range(4):
                    wd_copy(i, s).start()
                return c
            lax.fori_loop(0, chunks, issue, 0)
            arrived(*x_ex(1), 0)
            push(*x_ex(1), 2).start()

        w_copy(j, 0).wait()
        w_copy(j, 1).wait()
        gate_up(0, j)
        push(*a_ex(0, j), 0).start()
        push(*a_ex(0, j), 1).start()
        return carry

    lax.fori_loop(0, chunks, first_pass, 0)

    arrived(*x_ex(1), 1)
    arrived(*x_ex(1), 2)
    normalise(xbuf, 0, *PASSES[1])

    def second_pass(j, with_down):
        relay(0, j)
        if with_down:
            down_wait(0, j - 1, True)
        gate_up(1, j)
        if with_down:
            down(0, j - 1)
        push(*a_ex(1, j), 0).start()
        push(*a_ex(1, j), 1).start()

    def second_pass_step(j, carry):
        second_pass(j, True)

        @pl.when(j < q_slabs)
        def _():
            wq_copy(j).start()
        return carry

    second_pass(0, False)
    wq_copy(0).start()
    lax.fori_loop(1, chunks, second_pass_step, 0)

    def late_push(j, carry):
        push(*a_ex(2, j), 0).start()
        push(*a_ex(2, j), 1).start()
        return carry

    lax.fori_loop(0, chunks, late_push, 0)
    down_wait(0, chunks - 1, True)
    down(0, chunks - 1)
    y_copy(0).start()

    def relays(g, lo, hi):
        def step(j, carry):
            relay(g, j)
            return carry
        lax.fori_loop(lo, hi, step, 0)

    def downs(g, lo, hi, n):
        def step(b, carry):
            j = lo + b * n
            for i in range(n):
                down_wait(g, j + i, False)
            down(g, j, n)
            return carry
        lax.fori_loop(0, (hi - lo) // n, step, 0)

    def residual(g):
        y_copy(g).wait_recv()
        t0, m = GROUPS[g]
        for t in range(t0, t0 + m, 16):
            rows = slice(t, t + 16)
            v = (xbuf[row, rows, :].astype(F32) + (acc[rows, :] + ybuf[rows, :])).astype(BF16)
            xpbuf[row, rows, :] = v
            xo[rows, :] = v
        push(*p_ex(g), 0).start()
        push(*p_ex(g), 1).start()

    def residual_relay(g):
        arrived(*p_ex(g), 0)
        push(*p_ex(g), 2).start()

    def qkv(groups):
        for g in groups:
            arrived(*p_ex(g), 1)
            arrived(*p_ex(g), 2)
            normalise(xpbuf, 1, *GROUPS[g])
        t0 = GROUPS[groups[0]][0]
        m = sum(GROUPS[g][1] for g in groups)

        def step(i, carry):
            n = nbuf[t0:t0 + m, :]
            for s in range(2):
                j = 2 * i + s
                out = jnp.dot(n, wgu[j, 0], preferred_element_type=F32)
                qo[t0:t0 + m, pl.ds(pl.multiple_of(j * CB, CB), CB)] = out.astype(BF16)
            return carry
        lax.fori_loop(0, q_slabs // 2, step, 0)

    relays(1, 0, chunks)
    downs(1, 0, chunks, 4)
    y_copy(1).start()

    half = chunks // 2
    relays(2, 0, half)
    downs(2, 0, half, 2)
    residual(0)
    relays(2, half, chunks)
    downs(2, half, chunks, 2)
    y_copy(2).start()

    residual_relay(0)
    residual(1)

    def drain(j, carry):
        for g in range(3):
            for kind in range(3):
                push(*a_ex(g, j), kind).wait_send()
        return carry
    lax.fori_loop(0, chunks, drain, 0)
    for kind in range(3):
        push(*g_ex, kind).wait_send()
        for p in range(2):
            push(*x_ex(p), kind).wait_send()
    for j in range(q_slabs):
        wq_copy(j).wait()

    residual_relay(1)
    residual(2)
    qkv((0, 1))
    residual_relay(2)
    qkv((2,))
    for g in range(3):
        y_copy(g).wait_send()
        for kind in range(3):
            push(*p_ex(g), kind).wait_send()


def solution(mesh):
    def per_device(residual, gain_mlp, gain_attn, w_gate, w_up, w_down, w_qkv):
        tokens, hid = residual.shape
        d_model, d_ff = w_gate.shape
        q_width = w_qkv.shape[1]
        chunks = d_ff // CB
        any_spec = pl.BlockSpec(memory_space=pl.ANY)
        vmem_spec = pl.BlockSpec(memory_space=pltpu.VMEM)
        dma = pltpu.SemaphoreType.DMA
        groups, passes = len(GROUPS), len(PASSES)
        return pl.pallas_call(
            kernel,
            name='block',
            out_shape=(jax.ShapeDtypeStruct((tokens, hid), BF16), jax.ShapeDtypeStruct((tokens, q_width), BF16)),
            in_specs=[any_spec] * 7,
            out_specs=(vmem_spec, vmem_spec),
            scratch_shapes=[
                pltpu.VMEM((chunks, 2, d_model, CB), BF16),
                pltpu.VMEM((chunks, 4 * CB, hid), BF16),
                pltpu.VMEM((chunks, 4, tokens, CB), BF16),
                pltpu.VMEM((4, tokens, hid), BF16),
                pltpu.VMEM((4, tokens, hid), BF16),
                pltpu.VMEM((tokens, d_model), BF16),
                pltpu.VMEM((tokens, hid), F32),
                pltpu.VMEM((tokens, hid), F32),
                pltpu.VMEM((4, 2, hid), F32),
                dma((3,)),
                dma((chunks, 2)),
                dma((chunks, 4)),
                dma((q_width // CB,)),
                dma((passes, 3)), dma((passes, 3)),
                dma((3,)), dma((3,)),
                dma((groups, chunks, 3)), dma((groups, chunks, 3)),
                dma((groups,)), dma((groups,)),
                dma((groups, 3)), dma((groups, 3)),
            ],
            compiler_params=pltpu.CompilerParams(collective_id=0, has_side_effects=True,
                                                 vmem_limit_bytes=67_043_328),
        )(residual, gain_mlp, gain_attn, w_gate, w_up, w_down, w_qkv)

    tok_spec, gain_spec = P('data', 'row'), P('row')
    wide_spec = P(None, ('col', 'row'))
    return jax.shard_map(
        per_device, mesh=mesh,
        in_specs=(tok_spec, gain_spec, gain_spec, wide_spec, wide_spec, P('col', 'row'), wide_spec),
        out_specs=(tok_spec, P('data', ('col', 'row'))), check_vma=False)
```

```python
import functools

import jax
import jax.numpy as jnp
from jax import lax
from jax.experimental import pallas as pl
from jax.experimental.pallas import tpu as pltpu
from jax.sharding import PartitionSpec as P

NORM_EPS = 1e-6
MESH = pl.DeviceIdType.MESH
F32 = jnp.float32
BF16 = jnp.bfloat16

CB = 256
PIECES = ((0, 64), (64, 64))
GROUPS = ((0, 64), (64, 32), (96, 32))
UNROLL = 2
AHEAD = 8


def kernel(res_h, g1_h, g2_h, wg_h, wu_h, wd_h, wq_h, xo, qo,
           wgu, wdb, abuf, xbuf, xpbuf, nbuf, acc, ybuf, gbuf,
           lsem, wsem, wdsem, wqsem, xs, xr, gs, gr, as_, ar, ys, yr, ps, pr):
    row, col = lax.axis_index('row'), lax.axis_index('col')
    mate = row + 1 - 2 * lax.rem(row, 2)
    near = lax.rem(row + 2, 4)
    far = lax.rem(mate + 2, 4)
    d_ff = wg_h.shape[1]
    chunks = d_ff // CB
    hid = res_h.shape[1]
    d_model = 4 * hid
    q_slabs = wq_h.shape[1] // CB

    def remote(src, dst, send, recv, device):
        return pltpu.make_async_remote_copy(src_ref=src, dst_ref=dst, send_sem=send, recv_sem=recv,
                                            device_id=device, device_id_type=MESH)

    def push(at, send, recv, kind):
        slot = (row, row, near)[kind]
        return remote(at(slot), at(slot), send(kind), recv(kind), {'row': (near, mate, mate)[kind]})

    def arrived(at, send, recv, kind):
        slot = (near, mate, far)[kind]
        remote(at(slot), at(slot), send(kind), recv(kind), {'row': mate}).wait_recv()

    def x_ex(p):
        t0, m = PIECES[p]
        return (lambda s: xbuf.at[s, pl.ds(t0, m)]), (lambda k: xs.at[p, k]), (lambda k: xr.at[p, k])

    g_ex = (lambda s: gbuf.at[s]), (lambda k: gs.at[k]), (lambda k: gr.at[k])

    def a_ex(g, j):
        t0, m = GROUPS[g]
        return (lambda s: abuf.at[j, s, pl.ds(t0, m)]), (lambda k: as_.at[g, k]), (lambda k: ar.at[g, j, k])

    def p_ex(g):
        t0, m = GROUPS[g]
        return (lambda s: xpbuf.at[s, pl.ds(t0, m)]), (lambda k: ps.at[g, k]), (lambda k: pr.at[g, k])

    def y_copy(g):
        rows = pl.ds(*GROUPS[g])
        return remote(acc.at[rows], ybuf.at[rows], ys.at[g], yr.at[g], {'col': 1 - col})

    def w_copy(j, half):
        src = (wg_h, wu_h)[half]
        start = j * CB if isinstance(j, int) else pl.multiple_of(j * CB, CB)
        return pltpu.make_async_copy(src.at[:, pl.ds(start, CB)], wgu.at[j, half], wsem.at[j, half])

    def wd_copy(j, s):
        start = pl.multiple_of(s * d_ff + j * CB, CB)
        return pltpu.make_async_copy(wd_h.at[pl.ds(start, CB)], wdb.at[j, pl.ds(s * CB, CB)], wdsem.at[j, s])

    def wq_copy(j):
        return pltpu.make_async_copy(wq_h.at[:, pl.ds(pl.multiple_of(j * CB, CB), CB)], wgu.at[j, 0], wqsem.at[j])

    loads = [pltpu.make_async_copy(res_h, xbuf.at[row], lsem.at[0]),
             pltpu.make_async_copy(g1_h, gbuf.at[row, 0], lsem.at[1]),
             pltpu.make_async_copy(g2_h, gbuf.at[row, 1], lsem.at[2])]
    for copy in loads:
        copy.start()
    barrier = pltpu.get_barrier_semaphore()
    for device in ({'row': mate}, {'row': near}, {'col': 1 - col}):
        pl.semaphore_signal(barrier, inc=1, device_id=device, device_id_type=MESH)
    with jax.named_scope('loads'):
        for copy in loads:
            copy.wait()
    for j in range(AHEAD):
        w_copy(j, 0).start()
        w_copy(j, 1).start()
    acc[...] = jnp.zeros_like(acc)
    with jax.named_scope('barrier'):
        pl.semaphore_wait(barrier, 3)

    push(*x_ex(0), 0).start()
    push(*g_ex, 0).start()
    push(*x_ex(0), 1).start()
    push(*g_ex, 1).start()
    push(*x_ex(1), 0).start()
    push(*x_ex(1), 1).start()

    def normalise(src, which, t0, m):
        step = 16
        scales = []
        for t in range(t0, t0 + m, step):
            total = jnp.zeros((step, hid), F32)
            for q in range(4):
                v = src[q, t:t + step, :].astype(F32)
                total = total + v * v
            scales.append(lax.rsqrt(jnp.sum(total, axis=1, keepdims=True) / d_model + NORM_EPS))
        for i, t in enumerate(range(t0, t0 + m, step)):
            for q in range(4):
                v = src[q, t:t + step, :].astype(F32)
                nbuf[t:t + step, q * hid:(q + 1) * hid] = (v * scales[i] * gbuf[q, which:which + 1, :]).astype(BF16)

    with jax.named_scope('xnear'):
        arrived(*g_ex, 0)
        push(*g_ex, 2).start()
        arrived(*x_ex(0), 0)
        push(*x_ex(0), 2).start()
    with jax.named_scope('xfar'):
        for kind in (1, 2):
            arrived(*g_ex, kind)
            arrived(*x_ex(0), kind)
    with jax.named_scope('norm0'):
        normalise(xbuf, 0, *PIECES[0])
    with jax.named_scope('xnear1'):
        arrived(*x_ex(1), 0)
        push(*x_ex(1), 2).start()
    with jax.named_scope('xfar1'):
        for kind in (1, 2):
            arrived(*x_ex(1), kind)
    with jax.named_scope('norm1'):
        normalise(xbuf, 0, *PIECES[1])

    def gate_up(j):
        n = nbuf[...]
        gate = jnp.dot(n, wgu[j, 0], preferred_element_type=F32)
        up = jnp.dot(n, wgu[j, 1], preferred_element_type=F32)
        abuf[j, row] = (jax.nn.silu(gate) * up).astype(BF16)

    def relay(g, j):
        arrived(*a_ex(g, j), 0)
        push(*a_ex(g, j), 2).start()

    def down_wait(g, j, first):
        arrived(*a_ex(g, j), 1)
        arrived(*a_ex(g, j), 2)
        if first:
            for s in range(4):
                wd_copy(j, s).wait()

    def down(g, j, n=1):
        t0, m = GROUPS[g]
        a = jnp.concatenate([abuf[j + i, s, t0:t0 + m, :] for i in range(n) for s in range(4)], axis=1)
        w = wdb[pl.ds(j, n)].reshape(n * 4 * CB, hid)
        acc[t0:t0 + m, :] += jnp.dot(a, w, preferred_element_type=F32)

    def gate_up_step(b, carry):
        first = b * UNROLL

        @pl.when(first + AHEAD < chunks)
        def _():
            for i in range(UNROLL):
                w_copy(first + i + AHEAD, 0).start()
                w_copy(first + i + AHEAD, 1).start()

        @pl.when(first == chunks - AHEAD)
        def _():
            def issue(i, c):
                for s in range(4):
                    wd_copy(i, s).start()
                return c
            lax.fori_loop(0, chunks, issue, 0)

        with jax.named_scope('wwait'):
            for i in range(UNROLL):
                w_copy(first + i, 0).wait()
                w_copy(first + i, 1).wait()
        with jax.named_scope('gateup'):
            for i in range(UNROLL):
                gate_up(first + i)
                push(*a_ex(0, first + i), 0).start()
                push(*a_ex(0, first + i), 1).start()
        return carry

    lax.fori_loop(0, chunks // UNROLL, gate_up_step, 0)

    for g in (1, 2):
        def late_push(j, carry):
            push(*a_ex(g, j), 0).start()
            push(*a_ex(g, j), 1).start()
            return carry
        lax.fori_loop(0, chunks, late_push, 0)
    for j in range(q_slabs):
        wq_copy(j).start()

    def relay_down(g, lo, hi, n):
        first = g == 0

        def relays(b):
            for i in range(n):
                relay(g, b * n + i)

        def downs(b):
            for i in range(n):
                down_wait(g, b * n + i, first)
            down(g, b * n, n)

        def step(b, carry):
            with jax.named_scope(f'relay{g}'):
                relays(b)
            with jax.named_scope(f'down{g}'):
                downs(b - 1)
            return carry

        with jax.named_scope(f'relay{g}'):
            relays(lo // n)
        lax.fori_loop(lo // n + 1, hi // n, step, 0)
        with jax.named_scope(f'down{g}'):
            downs(hi // n - 1)

    def residual(g):
        y_copy(g).wait_recv()
        t0, m = GROUPS[g]
        for t in range(t0, t0 + m, 16):
            rows = slice(t, t + 16)
            v = (xbuf[row, rows, :].astype(F32) + (acc[rows, :] + ybuf[rows, :])).astype(BF16)
            xpbuf[row, rows, :] = v
            xo[rows, :] = v
        push(*p_ex(g), 0).start()
        push(*p_ex(g), 1).start()

    def residual_relay(g):
        arrived(*p_ex(g), 0)
        push(*p_ex(g), 2).start()

    def qkv(groups):
        for g in groups:
            arrived(*p_ex(g), 1)
            arrived(*p_ex(g), 2)
            normalise(xpbuf, 1, *GROUPS[g])
        t0 = GROUPS[groups[0]][0]
        m = sum(GROUPS[g][1] for g in groups)

        def step(i, carry):
            n = nbuf[t0:t0 + m, :]
            for s in range(2):
                j = 2 * i + s
                out = jnp.dot(n, wgu[j, 0], preferred_element_type=F32)
                qo[t0:t0 + m, pl.ds(pl.multiple_of(j * CB, CB), CB)] = out.astype(BF16)
            return carry
        lax.fori_loop(0, q_slabs // 2, step, 0)

    relay_down(0, 0, chunks, 2)
    y_copy(0).start()
    relay_down(1, 0, chunks, 2)
    y_copy(1).start()
    half = chunks // 2
    relay_down(2, 0, half, 2)
    with jax.named_scope('resid0'):
        residual(0)
    relay_down(2, half, chunks, 2)
    y_copy(2).start()

    with jax.named_scope('rrelay0'):
        residual_relay(0)
    with jax.named_scope('resid1'):
        residual(1)

    with jax.named_scope('drain'):
        for kind in range(3):
            push(*g_ex, kind).wait_send()
            for p in range(2):
                push(*x_ex(p), kind).wait_send()
            for g in range(3):
                push(*a_ex(g, slice(None)), kind).wait_send()
        for j in range(q_slabs):
            wq_copy(j).wait()

    with jax.named_scope('rrelay1'):
        residual_relay(1)
    with jax.named_scope('resid2'):
        residual(2)
    with jax.named_scope('qkv01'):
        qkv((0, 1))
    with jax.named_scope('rrelay2'):
        residual_relay(2)
    with jax.named_scope('qkv2'):
        qkv((2,))
    with jax.named_scope('end'):
        for g in range(3):
            y_copy(g).wait_send()
            for kind in range(3):
                push(*p_ex(g), kind).wait_send()


def solution(mesh):
    def per_device(residual, gain_mlp, gain_attn, w_gate, w_up, w_down, w_qkv):
        tokens, hid = residual.shape
        d_model, d_ff = w_gate.shape
        q_width = w_qkv.shape[1]
        chunks = d_ff // CB
        any_spec = pl.BlockSpec(memory_space=pl.ANY)
        vmem_spec = pl.BlockSpec(memory_space=pltpu.VMEM)
        dma = pltpu.SemaphoreType.DMA
        groups, pieces = len(GROUPS), len(PIECES)
        return pl.pallas_call(
            kernel,
            name='block',
            out_shape=(pltpu.VMEM((tokens, hid), BF16), pltpu.VMEM((tokens, q_width), BF16)),
            in_specs=[any_spec] * 7,
            out_specs=(vmem_spec, vmem_spec),
            scratch_shapes=[
                pltpu.VMEM((chunks, 2, d_model, CB), BF16),
                pltpu.VMEM((chunks, 4 * CB, hid), BF16),
                pltpu.VMEM((chunks, 4, tokens, CB), BF16),
                pltpu.VMEM((4, tokens, hid), BF16),
                pltpu.VMEM((4, tokens, hid), BF16),
                pltpu.VMEM((tokens, d_model), BF16),
                pltpu.VMEM((tokens, hid), F32),
                pltpu.VMEM((tokens, hid), F32),
                pltpu.VMEM((4, 2, hid), F32),
                dma((3,)),
                dma((chunks, 2)),
                dma((chunks, 4)),
                dma((q_width // CB,)),
                dma((pieces, 3)), dma((pieces, 3)),
                dma((3,)), dma((3,)),
                dma((groups, 3)), dma((groups, chunks, 3)),
                dma((groups,)), dma((groups,)),
                dma((groups, 3)), dma((groups, 3)),
            ],
            compiler_params=pltpu.CompilerParams(collective_id=0, has_side_effects=True,
                                                 vmem_limit_bytes=66_400_000),
        )(residual, gain_mlp, gain_attn, w_gate, w_up, w_down, w_qkv)

    tok_spec, gain_spec = P('data', 'row'), P('row')
    wide_spec = P(None, ('col', 'row'))
    return jax.shard_map(
        per_device, mesh=mesh,
        in_specs=(tok_spec, gain_spec, gain_spec, wide_spec, wide_spec, P('col', 'row'), wide_spec),
        out_specs=(tok_spec, P('data', ('col', 'row'))), check_vma=False)
```

```python
import functools

import jax
import jax.numpy as jnp
from jax import lax
from jax.experimental import pallas as pl
from jax.experimental.pallas import tpu as pltpu
from jax.sharding import PartitionSpec as P

NORM_EPS = 1e-6
MESH = pl.DeviceIdType.MESH
F32 = jnp.float32
BF16 = jnp.bfloat16

CB = 256
PIECES = ((0, 64), (64, 64))
GROUPS = ((0, 64), (64, 32), (96, 32))
BLK = 2
EARLY = 4
STEP = 4
AHEAD = 6


def kernel(res_h, g1_h, g2_h, wg_h, wu_h, wd_h, wq_h, xo, qo,
           wgu, wdb, abuf, xbuf, xpbuf, nbuf, acc, ybuf, gbuf,
           lsem, wsem, wdsem, wqsem, xs, xr, gs, gr, as_, ar, ys, yr, ps, pr):
    row, col = lax.axis_index('row'), lax.axis_index('col')
    mate = row + 1 - 2 * lax.rem(row, 2)
    near = lax.rem(row + 2, 4)
    far = lax.rem(mate + 2, 4)
    d_ff = wg_h.shape[1]
    chunks = d_ff // CB
    hid = res_h.shape[1]
    d_model = 4 * hid
    q_slabs = wq_h.shape[1] // CB

    def remote(src, dst, send, recv, device):
        return pltpu.make_async_remote_copy(src_ref=src, dst_ref=dst, send_sem=send, recv_sem=recv,
                                            device_id=device, device_id_type=MESH)

    def push(at, send, recv, kind):
        slot = (row, row, near)[kind]
        return remote(at(slot), at(slot), send(kind), recv(kind), {'row': (near, mate, mate)[kind]})

    def arrived(at, send, recv, kind):
        slot = (near, mate, far)[kind]
        remote(at(slot), at(slot), send(kind), recv(kind), {'row': mate}).wait_recv()

    def x_ex(p):
        t0, m = PIECES[p]
        return (lambda s: xbuf.at[s, pl.ds(t0, m)]), (lambda k: xs), (lambda k: xr.at[p, k])

    g_ex = (lambda s: gbuf.at[s]), (lambda k: gs), (lambda k: gr.at[k])

    def a_ex(g, j, b, n=1):
        t0, m = GROUPS[g]
        return (lambda s: abuf.at[pl.ds(j, n), s, pl.ds(t0, m)]), (lambda k: as_), (lambda k: ar.at[g, b, k])

    def p_ex(g):
        t0, m = GROUPS[g]
        return (lambda s: xpbuf.at[s, pl.ds(t0, m)]), (lambda k: ps), (lambda k: pr.at[g, k])

    def sent(buf, sem):
        remote(buf, buf, sem, sem, {'row': mate}).wait_send()

    def y_copy(g):
        rows = pl.ds(*GROUPS[g])
        return remote(acc.at[rows], ybuf.at[rows], ys, yr.at[g], {'col': 1 - col})

    def w_start(j):
        for half, src in enumerate((wg_h, wu_h)):
            pltpu.make_async_copy(src.at[:, pl.ds(j * CB, CB)], wgu.at[j, half], wsem.at[j]).start()

    def w_wait(j):
        pltpu.make_async_copy(wgu.at[j], wgu.at[j], wsem.at[j]).wait()

    def wd_start(b):
        for j in range(b * 2 * BLK, (b + 1) * 2 * BLK):
            for s in range(4):
                pltpu.make_async_copy(wd_h.at[pl.ds(s * d_ff + j * CB, CB)], wdb.at[j, pl.ds(s * CB, CB)],
                                      wdsem.at[b]).start()

    def wd_wait(b):
        part = wdb.at[pl.ds(b * 2 * BLK, 2 * BLK)]
        pltpu.make_async_copy(part, part, wdsem.at[b]).wait()

    def wq_start():
        for j in range(q_slabs):
            pltpu.make_async_copy(wq_h.at[:, pl.ds(j * CB, CB)], wgu.at[j, 0], wqsem).start()

    def wq_wait():
        part = wgu.at[pl.ds(0, q_slabs), 0]
        pltpu.make_async_copy(part, part, wqsem).wait()

    loads = [pltpu.make_async_copy(res_h, xbuf.at[row], lsem.at[0]),
             pltpu.make_async_copy(g1_h, gbuf.at[row, 0], lsem.at[1]),
             pltpu.make_async_copy(g2_h, gbuf.at[row, 1], lsem.at[2])]
    for copy in loads:
        copy.start()
    barrier = pltpu.get_barrier_semaphore()
    for device in ({'row': mate}, {'row': near}, {'col': 1 - col}):
        pl.semaphore_signal(barrier, inc=1, device_id=device, device_id_type=MESH)
    with jax.named_scope('loads'):
        for copy in loads:
            copy.wait()
    for j in range(AHEAD):
        w_start(j)
    acc[...] = jnp.zeros_like(acc)
    with jax.named_scope('barrier'):
        pl.semaphore_wait(barrier, 3)

    push(*x_ex(0), 0).start()
    push(*g_ex, 0).start()
    push(*x_ex(0), 1).start()
    push(*g_ex, 1).start()
    push(*x_ex(1), 0).start()
    push(*x_ex(1), 1).start()

    def normalise(src, which, t0, m):
        step = 16
        scales = []
        for t in range(t0, t0 + m, step):
            total = jnp.zeros((step, hid), F32)
            for q in range(4):
                v = src[q, t:t + step, :].astype(F32)
                total = total + v * v
            scales.append(lax.rsqrt(jnp.sum(total, axis=1, keepdims=True) / d_model + NORM_EPS))
        for i, t in enumerate(range(t0, t0 + m, step)):
            for q in range(4):
                v = src[q, t:t + step, :].astype(F32)
                nbuf[t:t + step, q * hid:(q + 1) * hid] = (v * scales[i] * gbuf[q, which:which + 1, :]).astype(BF16)

    with jax.named_scope('w'):
        for j in range(EARLY):
            w_wait(j)
            w_start(AHEAD + j)

    def x_arrive(p):
        with jax.named_scope(f'xnear{p}'):
            if p == 0:
                arrived(*g_ex, 0)
                push(*g_ex, 2).start()
            arrived(*x_ex(p), 0)
            push(*x_ex(p), 2).start()
        with jax.named_scope(f'xfar{p}'):
            for kind in (1, 2):
                if p == 0:
                    arrived(*g_ex, kind)
                arrived(*x_ex(p), kind)
        with jax.named_scope(f'norm{p}'):
            normalise(xbuf, 0, *PIECES[p])

    def gate_up(j, t0, m):
        n = nbuf[t0:t0 + m, :]
        gate = jnp.dot(n, wgu[j, 0], preferred_element_type=F32)
        up = jnp.dot(n, wgu[j, 1], preferred_element_type=F32)
        abuf[j, row, t0:t0 + m, :] = (jax.nn.silu(gate) * up).astype(BF16)

    def a_push(g, j):
        push(*a_ex(g, j, j // BLK), 0).start()
        push(*a_ex(g, j, j // BLK), 1).start()

    def relay(g, b):
        with jax.named_scope(f'relay{g}#b={b}'):
            arrived(*a_ex(g, b * BLK, b, BLK), 0)
            push(*a_ex(g, b * BLK, b, BLK), 2).start()

    def down(g, b, n=1):
        with jax.named_scope(f'dwait{g}#b={b}'):
            for i in range(b, b + n):
                arrived(*a_ex(g, i * BLK, i, BLK), 1)
                arrived(*a_ex(g, i * BLK, i, BLK), 2)
            if g == 0:
                wd_wait(b // 2)
        with jax.named_scope(f'down{g}#b={b}'):
            t0, m = GROUPS[g]
            js = range(b * BLK, (b + n) * BLK)
            a = jnp.concatenate([abuf[j, s, t0:t0 + m, :] for j in js for s in range(4)], axis=1)
            w = wdb[js[0]:js[-1] + 1].reshape(len(js) * 4 * CB, hid)
            acc[t0:t0 + m, :] += jnp.dot(a, w, preferred_element_type=F32)

    x_arrive(0)
    w_start(AHEAD + EARLY)
    w_start(AHEAD + EARLY + 1)
    with jax.named_scope('gu0'):
        for j in range(EARLY):
            gate_up(j, *PIECES[0])
            a_push(0, j)
    x_arrive(1)
    for b in range(chunks // (2 * BLK)):
        wd_start(b)
    with jax.named_scope('gu1'):
        for j in range(EARLY):
            gate_up(j, *PIECES[1])
            a_push(1, j)
    for i, first in enumerate(range(EARLY, chunks, STEP)):
        if i:
            relay(0, 0)
        with jax.named_scope('wwait'):
            for j in range(first, first + STEP):
                w_wait(j)
        with jax.named_scope('gu'):
            for j in range(first, first + STEP):
                gate_up(j, 0, nbuf.shape[0])
                a_push(0, j)
    wq_start()
    for j in range(EARLY, chunks):
        a_push(1, j)
    for j in range(chunks):
        a_push(2, j)

    def residual(g):
        y_copy(g).wait_recv()
        t0, m = GROUPS[g]
        for t in range(t0, t0 + m, 16):
            rows = slice(t, t + 16)
            v = (xbuf[row, rows, :].astype(F32) + (acc[rows, :] + ybuf[rows, :])).astype(BF16)
            xpbuf[row, rows, :] = v
            xo[rows, :] = v
        push(*p_ex(g), 0).start()
        push(*p_ex(g), 1).start()

    def residual_relay(g):
        arrived(*p_ex(g), 0)
        push(*p_ex(g), 2).start()

    def qkv(groups):
        for g in groups:
            arrived(*p_ex(g), 1)
            arrived(*p_ex(g), 2)
            normalise(xpbuf, 1, *GROUPS[g])
        t0 = GROUPS[groups[0]][0]
        m = sum(GROUPS[g][1] for g in groups)

        n = nbuf[t0:t0 + m, :]
        for j in range(q_slabs):
            out = jnp.dot(n, wgu[j, 0], preferred_element_type=F32)
            qo[t0:t0 + m, j * CB:(j + 1) * CB] = out.astype(BF16)

    relay(0, 1)
    relay(1, 0)
    relay(0, 2)
    relay(1, 1)
    down(0, 0, 2)
    relay(0, 3)
    relay(0, 4)
    down(0, 2, 2)
    relay(0, 5)
    relay(1, 2)
    down(0, 4, 2)
    y_copy(0).start()
    relay(1, 3)
    down(1, 0, 2)
    relay(1, 4)
    relay(1, 5)
    down(1, 2, 2)
    relay(2, 0)
    relay(2, 1)
    down(1, 4, 2)
    y_copy(1).start()
    relay(2, 2)
    down(2, 0, 2)
    with jax.named_scope('resid0'):
        residual(0)
    relay(2, 3)
    relay(2, 4)
    down(2, 2, 2)
    relay(2, 5)
    down(2, 4)
    down(2, 5)
    y_copy(2).start()

    with jax.named_scope('rrelay0'):
        residual_relay(0)
    with jax.named_scope('resid1'):
        residual(1)

    with jax.named_scope('drain'):
        sent(gbuf.at[pl.ds(0, 3)], gs)
        sent(xbuf.at[pl.ds(0, 3)], xs)
        sent(abuf.at[:, pl.ds(0, 3)], as_)
        wq_wait()

    with jax.named_scope('rrelay1'):
        residual_relay(1)
    with jax.named_scope('resid2'):
        residual(2)
    with jax.named_scope('qkv01'):
        qkv((0, 1))
    with jax.named_scope('rrelay2'):
        residual_relay(2)
    with jax.named_scope('qkv2'):
        qkv((2,))
    with jax.named_scope('end'):
        sent(acc, ys)
        sent(xpbuf.at[pl.ds(0, 3)], ps)


def solution(mesh):
    def per_device(residual, gain_mlp, gain_attn, w_gate, w_up, w_down, w_qkv):
        tokens, hid = residual.shape
        d_model, d_ff = w_gate.shape
        q_width = w_qkv.shape[1]
        chunks = d_ff // CB
        any_spec = pl.BlockSpec(memory_space=pl.ANY)
        vmem_spec = pl.BlockSpec(memory_space=pltpu.VMEM)
        dma = pltpu.SemaphoreType.DMA
        groups, pieces = len(GROUPS), len(PIECES)
        return pl.pallas_call(
            kernel,
            name='block',
            out_shape=(pltpu.VMEM((tokens, hid), BF16), pltpu.VMEM((tokens, q_width), BF16)),
            in_specs=[any_spec] * 7,
            out_specs=(vmem_spec, vmem_spec),
            scratch_shapes=[
                pltpu.VMEM((chunks, 2, d_model, CB), BF16),
                pltpu.VMEM((chunks, 4 * CB, hid), BF16),
                pltpu.VMEM((chunks, 4, tokens, CB), BF16),
                pltpu.VMEM((4, tokens, hid), BF16),
                pltpu.VMEM((4, tokens, hid), BF16),
                pltpu.VMEM((tokens, d_model), BF16),
                pltpu.VMEM((tokens, hid), F32),
                pltpu.VMEM((tokens, hid), F32),
                pltpu.VMEM((4, 2, hid), F32),
                dma((3,)),
                dma((chunks,)),
                dma((chunks // (2 * BLK),)),
                dma,
                dma, dma((pieces, 3)),
                dma, dma((3,)),
                dma, dma((groups, chunks // BLK, 3)),
                dma, dma((groups,)),
                dma, dma((groups, 3)),
            ],
            compiler_params=pltpu.CompilerParams(collective_id=0, has_side_effects=True,
                                                 vmem_limit_bytes=66_400_000),
        )(residual, gain_mlp, gain_attn, w_gate, w_up, w_down, w_qkv)

    tok_spec, gain_spec = P('data', 'row'), P('row')
    wide_spec = P(None, ('col', 'row'))
    return jax.shard_map(
        per_device, mesh=mesh,
        in_specs=(tok_spec, gain_spec, gain_spec, wide_spec, wide_spec, P('col', 'row'), wide_spec),
        out_specs=(tok_spec, P('data', ('col', 'row'))), check_vma=False)
```

```python
import functools

import jax
import jax.numpy as jnp
from jax import lax
from jax.experimental import pallas as pl
from jax.experimental.pallas import tpu as pltpu
from jax.sharding import PartitionSpec as P

NORM_EPS = 1e-6
MESH = pl.DeviceIdType.MESH
F32 = jnp.float32
BF16 = jnp.bfloat16

CB = 256
PIECES = ((0, 64), (64, 64))
GROUPS = ((0, 64), (64, 32), (96, 32))
PAD = 16
BLK = 2
EARLY = 4
STEP = 4
AHEAD = 5


def kernel(res_h, g1_h, g2_h, wg_h, wu_h, wd_h, wq_h, xo, qo,
           wgu, wdb, abuf, xbuf, xpbuf, nbuf, acc, ybuf, gbuf,
           lsem, wsem, wdsem, wqsem, xs, xr, gs, gr, as_, ar, ys, yr, ps, pr):
    row, col = lax.axis_index('row'), lax.axis_index('col')
    mate = row + 1 - 2 * lax.rem(row, 2)
    near = lax.rem(row + 2, 4)
    far = lax.rem(mate + 2, 4)
    d_ff = wg_h.shape[1]
    chunks = d_ff // CB
    hid = res_h.shape[1]
    d_model = 4 * hid
    q_slabs = wq_h.shape[1] // CB

    def remote(src, dst, send, recv, device):
        return pltpu.make_async_remote_copy(src_ref=src, dst_ref=dst, send_sem=send, recv_sem=recv,
                                            device_id=device, device_id_type=MESH)

    def push(at, send, recv, kind):
        slot = (row, row, near)[kind]
        return remote(at(slot), at(slot), send(kind), recv(kind), {'row': (near, mate, mate)[kind]})

    def arrived(at, send, recv, kind):
        slot = (near, mate, far)[kind]
        remote(at(slot), at(slot), send(kind), recv(kind), {'row': mate}).wait_recv()

    def x_ex(p):
        t0, m = PIECES[p]
        return (lambda s: xbuf.at[s, pl.ds(t0, m)]), (lambda k: xs), (lambda k: xr.at[p, k])

    g_ex = (lambda s: gbuf.at[s]), (lambda k: gs), (lambda k: gr.at[k])

    def a_ex(g, j, b, n=1):
        t0, m = GROUPS[g]
        return (lambda s: abuf.at[pl.ds(j, n), s, pl.ds(t0, m)]), (lambda k: as_), (lambda k: ar.at[g, b, k])

    def p_ex(g):
        t0, m = GROUPS[g]
        return (lambda s: xpbuf.at[s, pl.ds(t0, m)]), (lambda k: ps), (lambda k: pr.at[g, k])

    def sent(buf, sem):
        remote(buf, buf, sem, sem, {'row': mate}).wait_send()

    def y_copy(g):
        rows = pl.ds(*GROUPS[g])
        return remote(acc.at[0, rows], ybuf.at[rows], ys, yr.at[g], {'col': 1 - col})

    def gu_part(j, half):
        return wgu.at[j, pl.ds(half * (d_model + PAD), d_model)]

    def w_start(j):
        for half, src in enumerate((wg_h, wu_h)):
            pltpu.make_async_copy(src.at[:, pl.ds(j * CB, CB)], gu_part(j, half), wsem.at[j]).start()

    def w_wait(j):
        both = wgu.at[j, pl.ds(0, 2 * d_model)]
        pltpu.make_async_copy(both, both, wsem.at[j]).wait()

    def wd_start(b):
        for j in range(b * 2 * BLK, (b + 1) * 2 * BLK):
            for s in range(4):
                pltpu.make_async_copy(wd_h.at[pl.ds(s * d_ff + j * CB, CB)], wdb.at[j, pl.ds(s * CB, CB)],
                                      wdsem.at[b]).start()

    def wd_wait(b):
        part = wdb.at[pl.ds(b * 2 * BLK, 2 * BLK), pl.ds(0, 4 * CB)]
        pltpu.make_async_copy(part, part, wdsem.at[b]).wait()

    def wq_start():
        for j in range(q_slabs):
            pltpu.make_async_copy(wq_h.at[:, pl.ds(j * CB, CB)], gu_part(j, 0), wqsem).start()

    def wq_wait():
        part = wgu.at[pl.ds(0, q_slabs), pl.ds(0, d_model)]
        pltpu.make_async_copy(part, part, wqsem).wait()

    loads = [pltpu.make_async_copy(res_h, xbuf.at[row], lsem.at[0]),
             pltpu.make_async_copy(g1_h, gbuf.at[row, 0], lsem.at[1]),
             pltpu.make_async_copy(g2_h, gbuf.at[row, 1], lsem.at[2])]
    for copy in loads:
        copy.start()
    barrier = pltpu.get_barrier_semaphore()
    for device in ({'row': mate}, {'row': near}, {'col': 1 - col}):
        pl.semaphore_signal(barrier, inc=1, device_id=device, device_id_type=MESH)
    with jax.named_scope('loads'):
        for copy in loads:
            copy.wait()
    for j in range(AHEAD):
        w_start(j)
    acc[...] = jnp.zeros_like(acc)
    with jax.named_scope('barrier'):
        pl.semaphore_wait(barrier, 3)

    push(*x_ex(0), 0).start()
    push(*g_ex, 0).start()
    push(*x_ex(0), 1).start()
    push(*g_ex, 1).start()
    push(*x_ex(1), 0).start()
    push(*x_ex(1), 1).start()

    def normalise(src, which, t0, m):
        step = 16
        scales = []
        for t in range(t0, t0 + m, step):
            total = jnp.zeros((step, hid), F32)
            for q in range(4):
                v = src[q, t:t + step, :].astype(F32)
                total = total + v * v
            scales.append(lax.rsqrt(jnp.sum(total, axis=1, keepdims=True) / d_model + NORM_EPS))
        for i, t in enumerate(range(t0, t0 + m, step)):
            for q in range(4):
                v = src[q, t:t + step, :].astype(F32)
                nbuf[t:t + step, q * hid:(q + 1) * hid] = (v * scales[i] * gbuf[q, which:which + 1, :]).astype(BF16)

    with jax.named_scope('w'):
        for j in range(EARLY):
            w_wait(j)
            w_start(AHEAD + j)

    def x_arrive(p):
        with jax.named_scope(f'xnear{p}'):
            if p == 0:
                arrived(*g_ex, 0)
                push(*g_ex, 2).start()
            arrived(*x_ex(p), 0)
            push(*x_ex(p), 2).start()
        with jax.named_scope(f'xfar{p}'):
            for kind in (1, 2):
                if p == 0:
                    arrived(*g_ex, kind)
                arrived(*x_ex(p), kind)
        with jax.named_scope(f'norm{p}'):
            normalise(xbuf, 0, *PIECES[p])

    def gate_up(j, t0, m):
        n = nbuf[t0:t0 + m, :]
        gate = jnp.dot(n, gu_part(j, 0)[...], preferred_element_type=F32)
        up = jnp.dot(n, gu_part(j, 1)[...], preferred_element_type=F32)
        abuf[j, row, t0:t0 + m, :] = (jax.nn.silu(gate) * up).astype(BF16)

    def a_push(g, j):
        push(*a_ex(g, j, j // BLK), 0).start()
        push(*a_ex(g, j, j // BLK), 1).start()

    def relay(g, b):
        with jax.named_scope(f'relay{g}#b={b}'):
            arrived(*a_ex(g, b * BLK, b, BLK), 0)
            push(*a_ex(g, b * BLK, b, BLK), 2).start()

    def down(g, b, n=1):
        with jax.named_scope(f'dwait{g}#b={b}'):
            for i in range(b, b + n):
                arrived(*a_ex(g, i * BLK, i, BLK), 1)
                arrived(*a_ex(g, i * BLK, i, BLK), 2)
            if g == 0:
                wd_wait(b // 2)
        with jax.named_scope(f'down{g}#b={b}'):
            t0, m = GROUPS[g]
            js = range(b * BLK, (b + n) * BLK)
            for c in range(hid // CB):
                cols = slice(c * CB, (c + 1) * CB)
                for odd in range(2):
                    a = jnp.concatenate([abuf[j, s, t0:t0 + m, :] for j in js[odd::2] for s in range(4)], axis=1)
                    w = jnp.concatenate([wdb[j, :4 * CB, cols] for j in js[odd::2]], axis=0)
                    acc[odd, t0:t0 + m, cols] += jnp.dot(a, w, preferred_element_type=F32)

    def down_total(g):
        rows = pl.ds(*GROUPS[g])
        acc[0, rows, :] += acc[1, rows, :]

    def early(p):
        def step(i, carry):
            for k in range(BLK):
                gate_up(BLK * i + k, *PIECES[p])
                a_push(p, BLK * i + k)
            return carry
        lax.fori_loop(0, EARLY // BLK, step, 0)

    x_arrive(0)
    w_start(AHEAD + EARLY)
    w_start(AHEAD + EARLY + 1)
    with jax.named_scope('gu0'):
        early(0)
    x_arrive(1)
    w_start(AHEAD + EARLY + 2)
    wd_start(0)
    with jax.named_scope('gu1'):
        early(1)
    for i, first in enumerate(range(EARLY, chunks, STEP)):
        if i:
            relay(0, 0)
        wd_start(i + 1)
        with jax.named_scope('wwait'):
            for j in range(first, first + STEP):
                w_wait(j)
        with jax.named_scope('gu'):
            for j in range(first, first + STEP):
                gate_up(j, 0, nbuf.shape[0])
                a_push(0, j)
    wq_start()
    for j in range(EARLY, chunks):
        a_push(1, j)
    for j in range(chunks):
        a_push(2, j)

    def residual(g):
        y_copy(g).wait_recv()
        t0, m = GROUPS[g]
        for t in range(t0, t0 + m, 16):
            rows = slice(t, t + 16)
            v = (xbuf[row, rows, :].astype(F32) + (acc[0, rows, :] + ybuf[rows, :])).astype(BF16)
            xpbuf[row, rows, :] = v
            xo[rows, :] = v
        push(*p_ex(g), 0).start()
        push(*p_ex(g), 1).start()

    def residual_relay(g):
        arrived(*p_ex(g), 0)
        push(*p_ex(g), 2).start()

    def qkv(groups):
        for g in groups:
            arrived(*p_ex(g), 1)
            arrived(*p_ex(g), 2)
            normalise(xpbuf, 1, *GROUPS[g])
        t0 = GROUPS[groups[0]][0]
        m = sum(GROUPS[g][1] for g in groups)

        def step(i, carry):
            n = nbuf[t0:t0 + m, :]
            for k in range(2):
                j = 2 * i + k
                out = jnp.dot(n, gu_part(j, 0)[...], preferred_element_type=F32)
                qo[t0:t0 + m, pl.ds(pl.multiple_of(j * CB, CB), CB)] = out.astype(BF16)
            return carry
        lax.fori_loop(0, q_slabs // 2, step, 0)

    relay(0, 1)
    relay(1, 0)
    relay(0, 2)
    relay(1, 1)
    down(0, 0, 2)
    relay(0, 3)
    relay(0, 4)
    down(0, 2, 2)
    relay(0, 5)
    relay(1, 2)
    down(0, 4, 2)
    down_total(0)
    y_copy(0).start()
    relay(1, 3)
    down(1, 0, 2)
    relay(1, 4)
    relay(1, 5)
    down(1, 2, 2)
    relay(2, 0)
    relay(2, 1)
    down(1, 4, 2)
    down_total(1)
    y_copy(1).start()
    relay(2, 2)
    down(2, 0, 2)
    with jax.named_scope('resid0'):
        residual(0)
    relay(2, 3)
    relay(2, 4)
    down(2, 2, 2)
    relay(2, 5)
    down(2, 4)
    down(2, 5)
    down_total(2)
    y_copy(2).start()

    with jax.named_scope('rrelay0'):
        residual_relay(0)
    with jax.named_scope('resid1'):
        residual(1)

    with jax.named_scope('drain'):
        sent(gbuf.at[pl.ds(0, 3)], gs)
        sent(xbuf.at[pl.ds(0, 3)], xs)
        sent(abuf.at[:, pl.ds(0, 3)], as_)
        wq_wait()

    with jax.named_scope('rrelay1'):
        residual_relay(1)
    with jax.named_scope('resid2'):
        residual(2)
    with jax.named_scope('qkv01'):
        qkv((0, 1))
    with jax.named_scope('rrelay2'):
        residual_relay(2)
    with jax.named_scope('qkv2'):
        qkv((2,))
    with jax.named_scope('end'):
        sent(acc.at[0], ys)
        sent(xpbuf.at[pl.ds(0, 3)], ps)


def solution(mesh):
    def per_device(residual, gain_mlp, gain_attn, w_gate, w_up, w_down, w_qkv):
        tokens, hid = residual.shape
        d_model, d_ff = w_gate.shape
        q_width = w_qkv.shape[1]
        chunks = d_ff // CB
        any_spec = pl.BlockSpec(memory_space=pl.ANY)
        vmem_spec = pl.BlockSpec(memory_space=pltpu.VMEM)
        dma = pltpu.SemaphoreType.DMA
        groups, pieces = len(GROUPS), len(PIECES)
        return pl.pallas_call(
            kernel,
            name='block',
            out_shape=(pltpu.VMEM((tokens, hid), BF16), pltpu.VMEM((tokens, q_width), BF16)),
            in_specs=[any_spec] * 7,
            out_specs=(vmem_spec, vmem_spec),
            scratch_shapes=[
                pltpu.VMEM((chunks, 2 * d_model + PAD, CB), BF16),
                pltpu.VMEM((chunks, 4 * CB + PAD, hid), BF16),
                pltpu.VMEM((chunks, 4, tokens, CB), BF16),
                pltpu.VMEM((4, tokens, hid), BF16),
                pltpu.VMEM((4, tokens, hid), BF16),
                pltpu.VMEM((tokens, d_model), BF16),
                pltpu.VMEM((2, tokens, hid), F32),
                pltpu.VMEM((tokens, hid), F32),
                pltpu.VMEM((4, 2, hid), F32),
                dma((3,)),
                dma((chunks,)),
                dma((chunks // (2 * BLK),)),
                dma,
                dma, dma((pieces, 3)),
                dma, dma((3,)),
                dma, dma((groups, chunks // BLK, 3)),
                dma, dma((groups,)),
                dma, dma((groups, 3)),
            ],
            compiler_params=pltpu.CompilerParams(collective_id=0, has_side_effects=True,
                                                 vmem_limit_bytes=66_400_000),
        )(residual, gain_mlp, gain_attn, w_gate, w_up, w_down, w_qkv)

    tok_spec, gain_spec = P('data', 'row'), P('row')
    wide_spec = P(None, ('col', 'row'))
    return jax.shard_map(
        per_device, mesh=mesh,
        in_specs=(tok_spec, gain_spec, gain_spec, wide_spec, wide_spec, P('col', 'row'), wide_spec),
        out_specs=(tok_spec, P('data', ('col', 'row'))), check_vma=False)
```

```python
import functools

import jax
import jax.numpy as jnp
from jax import lax
from jax.experimental import pallas as pl
from jax.experimental.pallas import tpu as pltpu
from jax.sharding import PartitionSpec as P

NORM_EPS = 1e-6
MESH = pl.DeviceIdType.MESH
F32 = jnp.float32
BF16 = jnp.bfloat16

CB = 256
PIECES = ((0, 64), (64, 64))
GROUPS = ((0, 64), (64, 32), (96, 32))
PAD = 16
BLK = 2
EARLY = 4
STEP = 4
AHEAD = 5


def kernel(res_h, g1_h, g2_h, wg_h, wu_h, wd_h, wq_h, xo, qo,
           wgu, wdb, abuf, xbuf, xpbuf, nbuf, acc, ybuf, gbuf,
           lsem, wsem, wdsem, wqsem, xs, xr, gs, gr, as_, ar, ys, yr, ps, pr):
    row, col = lax.axis_index('row'), lax.axis_index('col')
    mate = row + 1 - 2 * lax.rem(row, 2)
    near = lax.rem(row + 2, 4)
    far = lax.rem(mate + 2, 4)
    d_ff = wg_h.shape[1]
    chunks = d_ff // CB
    hid = res_h.shape[1]
    d_model = 4 * hid
    q_slabs = wq_h.shape[1] // CB

    def remote(src, dst, send, recv, device):
        return pltpu.make_async_remote_copy(src_ref=src, dst_ref=dst, send_sem=send, recv_sem=recv,
                                            device_id=device, device_id_type=MESH)

    def push(at, send, recv, kind, direct=False):
        slot = (row, row, row if direct else near)[kind]
        device = (near, mate, far if direct else mate)[kind]
        return remote(at(slot), at(slot), send(kind), recv(kind), {'row': device})

    def arrived(at, send, recv, kind):
        slot = (near, mate, far)[kind]
        remote(at(slot), at(slot), send(kind), recv(kind), {'row': mate}).wait_recv()

    def x_ex(p):
        t0, m = PIECES[p]
        return (lambda s: xbuf.at[s, pl.ds(t0, m)]), (lambda k: xs), (lambda k: xr.at[p, k])

    g_ex = (lambda s: gbuf.at[s]), (lambda k: gs), (lambda k: gr.at[k])

    def a_ex(g, j, b, n=1):
        t0, m = GROUPS[g]
        return (lambda s: abuf.at[pl.ds(j, n), s, pl.ds(t0, m)]), (lambda k: as_), (lambda k: ar.at[g, b, k])

    def p_ex(g):
        t0, m = GROUPS[g]
        return (lambda s: xpbuf.at[s, pl.ds(t0, m)]), (lambda k: ps), (lambda k: pr.at[g, k])

    def sent(buf, sem):
        remote(buf, buf, sem, sem, {'row': mate}).wait_send()

    def y_copy(g):
        rows = pl.ds(*GROUPS[g])
        return remote(acc.at[0, rows], ybuf.at[rows], ys, yr.at[g], {'col': 1 - col})

    def gu_part(j, half):
        return wgu.at[j, pl.ds(half * (d_model + PAD), d_model)]

    def w_start(j):
        for half, src in enumerate((wg_h, wu_h)):
            pltpu.make_async_copy(src.at[:, pl.ds(j * CB, CB)], gu_part(j, half), wsem.at[j]).start()

    def w_wait(j):
        both = wgu.at[j, pl.ds(0, 2 * d_model)]
        pltpu.make_async_copy(both, both, wsem.at[j]).wait()

    def wd_start(b):
        for j in range(b * 2 * BLK, (b + 1) * 2 * BLK):
            for s in range(4):
                pltpu.make_async_copy(wd_h.at[pl.ds(s * d_ff + j * CB, CB)], wdb.at[j, pl.ds(s * CB, CB)],
                                      wdsem.at[b]).start()

    def wd_wait(b):
        part = wdb.at[pl.ds(b * 2 * BLK, 2 * BLK), pl.ds(0, 4 * CB)]
        pltpu.make_async_copy(part, part, wdsem.at[b]).wait()

    def wq_start():
        for j in range(q_slabs):
            pltpu.make_async_copy(wq_h.at[:, pl.ds(j * CB, CB)], gu_part(j, 0), wqsem).start()

    def wq_wait():
        part = wgu.at[pl.ds(0, q_slabs), pl.ds(0, d_model)]
        pltpu.make_async_copy(part, part, wqsem).wait()

    loads = [pltpu.make_async_copy(res_h, xbuf.at[row], lsem.at[0]),
             pltpu.make_async_copy(g1_h, gbuf.at[row, 0], lsem.at[1]),
             pltpu.make_async_copy(g2_h, gbuf.at[row, 1], lsem.at[2])]
    for copy in loads:
        copy.start()
    barrier = pltpu.get_barrier_semaphore()
    for device in ({'row': mate}, {'row': near}, {'row': far}, {'col': 1 - col}):
        pl.semaphore_signal(barrier, inc=1, device_id=device, device_id_type=MESH)
    with jax.named_scope('loads'):
        for copy in loads:
            copy.wait()
    for j in range(AHEAD):
        w_start(j)
    acc[...] = jnp.zeros_like(acc)
    with jax.named_scope('barrier'):
        pl.semaphore_wait(barrier, 4)

    push(*x_ex(0), 0).start()
    push(*g_ex, 0).start()
    push(*x_ex(0), 1).start()
    push(*g_ex, 1).start()
    push(*x_ex(1), 0).start()
    push(*x_ex(1), 1).start()

    def normalise(src, which, t0, m):
        step = 16
        scales = []
        for t in range(t0, t0 + m, step):
            total = jnp.zeros((step, hid), F32)
            for q in range(4):
                v = src[q, t:t + step, :].astype(F32)
                total = total + v * v
            scales.append(lax.rsqrt(jnp.sum(total, axis=1, keepdims=True) / d_model + NORM_EPS))
        for i, t in enumerate(range(t0, t0 + m, step)):
            for q in range(4):
                v = src[q, t:t + step, :].astype(F32)
                nbuf[t:t + step, q * hid:(q + 1) * hid] = (v * scales[i] * gbuf[q, which:which + 1, :]).astype(BF16)

    with jax.named_scope('w'):
        for j in range(EARLY):
            w_wait(j)
            w_start(AHEAD + j)

    def x_relay(p):
        arrived(*x_ex(p), 0)
        push(*x_ex(p), 2).start()

    def x_norm(p):
        with jax.named_scope(f'xfar{p}'):
            for kind in (1, 2):
                if p == 0:
                    arrived(*g_ex, kind)
                arrived(*x_ex(p), kind)
        with jax.named_scope(f'norm{p}'):
            normalise(xbuf, 0, *PIECES[p])

    def gate_up(j, t0, m):
        n = nbuf[t0:t0 + m, :]
        gate = jnp.dot(n, gu_part(j, 0)[...], preferred_element_type=F32)
        up = jnp.dot(n, gu_part(j, 1)[...], preferred_element_type=F32)
        abuf[j, row, t0:t0 + m, :] = (jax.nn.silu(gate) * up).astype(BF16)

    def a_push(g, j):
        push(*a_ex(g, j, j // BLK), 0).start()
        push(*a_ex(g, j, j // BLK), 1).start()

    def relay(g, b):
        with jax.named_scope(f'relay{g}#b={b}'):
            arrived(*a_ex(g, b * BLK, b, BLK), 0)
            push(*a_ex(g, b * BLK, b, BLK), 2).start()

    def down(g, b, n=1):
        with jax.named_scope(f'dwait{g}#b={b}'):
            for i in range(b, b + n):
                arrived(*a_ex(g, i * BLK, i, BLK), 1)
                arrived(*a_ex(g, i * BLK, i, BLK), 2)
            if g == 0:
                wd_wait(b // 2)
        with jax.named_scope(f'down{g}#b={b}'):
            t0, m = GROUPS[g]
            js = range(b * BLK, (b + n) * BLK)
            for c in range(hid // CB):
                cols = slice(c * CB, (c + 1) * CB)
                for odd in range(2):
                    a = jnp.concatenate([abuf[j, s, t0:t0 + m, :] for j in js[odd::2] for s in range(4)], axis=1)
                    w = jnp.concatenate([wdb[j, :4 * CB, cols] for j in js[odd::2]], axis=0)
                    acc[odd, t0:t0 + m, cols] += jnp.dot(a, w, preferred_element_type=F32)

    def down_total(g):
        rows = pl.ds(*GROUPS[g])
        acc[0, rows, :] += acc[1, rows, :]

    def early(p):
        def step(i, carry):
            if p == 0:
                @pl.when(i == 1)
                def _():
                    x_relay(1)
            for k in range(BLK):
                gate_up(BLK * i + k, *PIECES[p])
                for g in (0,) if p == 0 else (1, 2):
                    a_push(g, BLK * i + k)
            return carry
        lax.fori_loop(0, EARLY // BLK, step, 0)

    with jax.named_scope('xnear0'):
        arrived(*g_ex, 0)
        push(*g_ex, 2).start()
        x_relay(0)
    x_norm(0)
    w_start(AHEAD + EARLY)
    w_start(AHEAD + EARLY + 1)
    with jax.named_scope('gu0'):
        early(0)
    x_norm(1)
    w_start(AHEAD + EARLY + 2)
    wd_start(0)
    with jax.named_scope('gu1'):
        early(1)
    for i, first in enumerate(range(EARLY, chunks, STEP)):
        for g, b in ((0, 0), (0, 1)) if i == 0 else ((1, 0), (1, 1)):
            relay(g, b)
        wd_start(i + 1)
        with jax.named_scope('wwait'):
            for j in range(first, first + STEP):
                w_wait(j)
        with jax.named_scope('gu'):
            for j in range(first, first + STEP):
                gate_up(j, 0, nbuf.shape[0])
                a_push(0, j)
    for g in (1, 2):
        for j in range(EARLY, chunks):
            a_push(g, j)
    wq_start()

    def residual(g):
        y_copy(g).wait_recv()
        t0, m = GROUPS[g]
        for t in range(t0, t0 + m, 16):
            rows = slice(t, t + 16)
            v = (xbuf[row, rows, :].astype(F32) + (acc[0, rows, :] + ybuf[rows, :])).astype(BF16)
            xpbuf[row, rows, :] = v
            xo[rows, :] = v
        push(*p_ex(g), 0).start()
        push(*p_ex(g), 1).start()
        if g == 2:
            push(*p_ex(g), 2, True).start()

    def residual_relay(g):
        arrived(*p_ex(g), 0)
        push(*p_ex(g), 2).start()

    def qkv(groups):
        for g in groups:
            arrived(*p_ex(g), 1)
            arrived(*p_ex(g), 2)
            normalise(xpbuf, 1, *GROUPS[g])
        t0 = GROUPS[groups[0]][0]
        m = sum(GROUPS[g][1] for g in groups)

        def step(i, carry):
            n = nbuf[t0:t0 + m, :]
            for k in range(2):
                j = 2 * i + k
                out = jnp.dot(n, gu_part(j, 0)[...], preferred_element_type=F32)
                qo[t0:t0 + m, pl.ds(pl.multiple_of(j * CB, CB), CB)] = out.astype(BF16)
            return carry
        lax.fori_loop(0, q_slabs // 2, step, 0)

    def finish(g):
        down_total(g)
        y_copy(g).start()

    relay(0, 2)
    relay(0, 3)
    relay(2, 0)
    relay(2, 1)
    down(0, 0, 2)
    down(0, 2, 2)
    relay(0, 4)
    down(1, 0, 2)
    relay(0, 5)
    relay(1, 2)
    down(0, 4, 2)
    finish(0)
    relay(1, 3)
    relay(1, 4)
    down(1, 2, 2)
    relay(1, 5)
    relay(2, 2)
    down(2, 0, 2)
    down(1, 4, 2)
    finish(1)
    relay(2, 3)
    relay(2, 4)
    relay(2, 5)
    down(2, 2, 2)
    down(2, 4, 2)
    finish(2)
    with jax.named_scope('drain'):
        sent(gbuf.at[pl.ds(0, 3)], gs)
        sent(xbuf.at[pl.ds(0, 3)], xs)
        sent(abuf.at[:, pl.ds(0, 3)], as_)
        wq_wait()
    with jax.named_scope('resid0'):
        residual(0)
    with jax.named_scope('resid1'):
        residual(1)
    with jax.named_scope('rrelay0'):
        residual_relay(0)
    with jax.named_scope('resid2'):
        residual(2)
    with jax.named_scope('rrelay1'):
        residual_relay(1)
    with jax.named_scope('qkv01'):
        qkv((0, 1))
    with jax.named_scope('xpwait'):
        arrived(*p_ex(2), 0)
    with jax.named_scope('qkv2'):
        qkv((2,))
    with jax.named_scope('end'):
        sent(acc.at[0], ys)
        sent(xpbuf.at[pl.ds(0, 3)], ps)


def solution(mesh):
    def per_device(residual, gain_mlp, gain_attn, w_gate, w_up, w_down, w_qkv):
        tokens, hid = residual.shape
        d_model, d_ff = w_gate.shape
        q_width = w_qkv.shape[1]
        chunks = d_ff // CB
        any_spec = pl.BlockSpec(memory_space=pl.ANY)
        vmem_spec = pl.BlockSpec(memory_space=pltpu.VMEM)
        dma = pltpu.SemaphoreType.DMA
        groups, pieces = len(GROUPS), len(PIECES)
        return pl.pallas_call(
            kernel,
            name='block',
            out_shape=(pltpu.VMEM((tokens, hid), BF16), pltpu.VMEM((tokens, q_width), BF16)),
            in_specs=[any_spec] * 7,
            out_specs=(vmem_spec, vmem_spec),
            scratch_shapes=[
                pltpu.VMEM((chunks, 2 * d_model + PAD, CB), BF16),
                pltpu.VMEM((chunks, 4 * CB + PAD, hid), BF16),
                pltpu.VMEM((chunks, 4, tokens, CB), BF16),
                pltpu.VMEM((4, tokens, hid), BF16),
                pltpu.VMEM((4, tokens, hid), BF16),
                pltpu.VMEM((tokens, d_model), BF16),
                pltpu.VMEM((2, tokens, hid), F32),
                pltpu.VMEM((tokens, hid), F32),
                pltpu.VMEM((4, 2, hid), F32),
                dma((3,)),
                dma((chunks,)),
                dma((chunks // (2 * BLK),)),
                dma,
                dma, dma((pieces, 3)),
                dma, dma((3,)),
                dma, dma((groups, chunks // BLK, 3)),
                dma, dma((groups,)),
                dma, dma((groups, 3)),
            ],
            compiler_params=pltpu.CompilerParams(collective_id=0, has_side_effects=True,
                                                 vmem_limit_bytes=66_400_000),
        )(residual, gain_mlp, gain_attn, w_gate, w_up, w_down, w_qkv)

    tok_spec, gain_spec = P('data', 'row'), P('row')
    wide_spec = P(None, ('col', 'row'))
    return jax.shard_map(
        per_device, mesh=mesh,
        in_specs=(tok_spec, gain_spec, gain_spec, wide_spec, wide_spec, P('col', 'row'), wide_spec),
        out_specs=(tok_spec, P('data', ('col', 'row'))), check_vma=False)
```

```python
import functools

import jax
import jax.numpy as jnp
from jax import lax
from jax.experimental import pallas as pl
from jax.experimental.pallas import tpu as pltpu
from jax.sharding import PartitionSpec as P

NORM_EPS = 1e-6
MESH = pl.DeviceIdType.MESH
F32 = jnp.float32
BF16 = jnp.bfloat16

CB = 256
PIECES = ((0, 64), (64, 64))
GROUPS = ((0, 64), (64, 48), (112, 16))
PAD = 16
BLK = 2
EARLY = 4
STEP = 4
AHEAD = 5


def kernel(res_h, g1_h, g2_h, wg_h, wu_h, wd_h, wq_h, xo, qo,
           wgu, wdb, abuf, xbuf, xpbuf, nbuf, acc, ybuf, gbuf,
           lsem, wsem, wdsem, wqsem, xs, xr, gs, gr, as_, ar, ys, yr, ps, pr):
    row, col = lax.axis_index('row'), lax.axis_index('col')
    mate = row + 1 - 2 * lax.rem(row, 2)
    near = lax.rem(row + 2, 4)
    far = lax.rem(mate + 2, 4)
    d_ff = wg_h.shape[1]
    chunks = d_ff // CB
    hid = res_h.shape[1]
    d_model = 4 * hid
    q_slabs = wq_h.shape[1] // CB

    def remote(src, dst, send, recv, device):
        return pltpu.make_async_remote_copy(src_ref=src, dst_ref=dst, send_sem=send, recv_sem=recv,
                                            device_id=device, device_id_type=MESH)

    def push(at, send, recv, kind, direct=False):
        slot = (row, row, row if direct else near)[kind]
        device = (near, mate, far if direct else mate)[kind]
        return remote(at(slot), at(slot), send(kind), recv(kind), {'row': device})

    def arrived(at, send, recv, kind):
        slot = (near, mate, far)[kind]
        remote(at(slot), at(slot), send(kind), recv(kind), {'row': mate}).wait_recv()

    def x_ex(p):
        t0, m = PIECES[p]
        return (lambda s: xbuf.at[s, pl.ds(t0, m)]), (lambda k: xs), (lambda k: xr.at[p, k])

    g_ex = (lambda s: gbuf.at[s]), (lambda k: gs), (lambda k: gr.at[k])

    def a_ex(g, j, b, n=1):
        t0, m = GROUPS[g]
        return (lambda s: abuf.at[pl.ds(j, n), s, pl.ds(t0, m)]), (lambda k: as_), (lambda k: ar.at[g, b, k])

    def p_ex(g):
        t0, m = GROUPS[g]
        return (lambda s: xpbuf.at[s, pl.ds(t0, m)]), (lambda k: ps), (lambda k: pr.at[g, k])

    def sent(buf, sem):
        remote(buf, buf, sem, sem, {'row': mate}).wait_send()

    def y_copy(g):
        rows = pl.ds(*GROUPS[g])
        return remote(acc.at[0, rows], ybuf.at[rows], ys, yr.at[g], {'col': 1 - col})

    def gu_part(j, half):
        return wgu.at[j, pl.ds(half * (d_model + PAD), d_model)]

    def w_start(j):
        for half, src in enumerate((wg_h, wu_h)):
            pltpu.make_async_copy(src.at[:, pl.ds(j * CB, CB)], gu_part(j, half), wsem.at[j]).start()

    def w_wait(j):
        both = wgu.at[j, pl.ds(0, 2 * d_model)]
        pltpu.make_async_copy(both, both, wsem.at[j]).wait()

    def wd_start(b):
        for j in range(b * 2 * BLK, (b + 1) * 2 * BLK):
            for s in range(4):
                pltpu.make_async_copy(wd_h.at[pl.ds(s * d_ff + j * CB, CB)], wdb.at[j, pl.ds(s * CB, CB)],
                                      wdsem.at[b]).start()

    def wd_wait(b):
        part = wdb.at[pl.ds(b * 2 * BLK, 2 * BLK), pl.ds(0, 4 * CB)]
        pltpu.make_async_copy(part, part, wdsem.at[b]).wait()

    def wq_start():
        for j in range(q_slabs):
            pltpu.make_async_copy(wq_h.at[:, pl.ds(j * CB, CB)], gu_part(j, 0), wqsem).start()

    def wq_wait():
        part = wgu.at[pl.ds(0, q_slabs), pl.ds(0, d_model)]
        pltpu.make_async_copy(part, part, wqsem).wait()

    loads = [pltpu.make_async_copy(res_h, xbuf.at[row], lsem.at[0]),
             pltpu.make_async_copy(g1_h, gbuf.at[row, 0], lsem.at[1]),
             pltpu.make_async_copy(g2_h, gbuf.at[row, 1], lsem.at[2])]
    for copy in loads:
        copy.start()
    barrier = pltpu.get_barrier_semaphore()
    for device in ({'row': mate}, {'row': near}, {'row': far}, {'col': 1 - col}):
        pl.semaphore_signal(barrier, inc=1, device_id=device, device_id_type=MESH)
    with jax.named_scope('loads'):
        for copy in loads:
            copy.wait()
    for j in range(AHEAD):
        w_start(j)
    acc[...] = jnp.zeros_like(acc)
    with jax.named_scope('barrier'):
        pl.semaphore_wait(barrier, 4)

    push(*x_ex(0), 0).start()
    push(*g_ex, 0).start()
    push(*x_ex(0), 1).start()
    push(*g_ex, 1).start()
    push(*x_ex(1), 0).start()
    push(*x_ex(1), 1).start()

    def normalise(src, which, t0, m):
        step = 16
        scales = []
        for t in range(t0, t0 + m, step):
            total = jnp.zeros((step, hid), F32)
            for q in range(4):
                v = src[q, t:t + step, :].astype(F32)
                total = total + v * v
            scales.append(lax.rsqrt(jnp.sum(total, axis=1, keepdims=True) / d_model + NORM_EPS))
        for i, t in enumerate(range(t0, t0 + m, step)):
            for q in range(4):
                v = src[q, t:t + step, :].astype(F32)
                nbuf[t:t + step, q * hid:(q + 1) * hid] = (v * scales[i] * gbuf[q, which:which + 1, :]).astype(BF16)

    with jax.named_scope('w'):
        for j in range(EARLY):
            w_wait(j)
            w_start(AHEAD + j)

    def x_relay(p):
        arrived(*x_ex(p), 0)
        push(*x_ex(p), 2).start()

    def x_norm(p):
        with jax.named_scope(f'xfar{p}'):
            for kind in (1, 2):
                if p == 0:
                    arrived(*g_ex, kind)
                arrived(*x_ex(p), kind)
        with jax.named_scope(f'norm{p}'):
            normalise(xbuf, 0, *PIECES[p])

    def gate_up(j, t0, m):
        n = nbuf[t0:t0 + m, :]
        gate = jnp.dot(n, gu_part(j, 0)[...], preferred_element_type=F32)
        up = jnp.dot(n, gu_part(j, 1)[...], preferred_element_type=F32)
        abuf[j, row, t0:t0 + m, :] = (jax.nn.silu(gate) * up).astype(BF16)

    def a_push(g, j):
        push(*a_ex(g, j, j // BLK), 0).start()
        push(*a_ex(g, j, j // BLK), 1).start()

    def relay(g, b):
        with jax.named_scope(f'relay{g}#b={b}'):
            arrived(*a_ex(g, b * BLK, b, BLK), 0)
            push(*a_ex(g, b * BLK, b, BLK), 2).start()

    def down(g, b, n=1):
        with jax.named_scope(f'dwait{g}#b={b}'):
            for i in range(b, b + n):
                arrived(*a_ex(g, i * BLK, i, BLK), 1)
                arrived(*a_ex(g, i * BLK, i, BLK), 2)
            if g == 0:
                wd_wait(b // 2)
        with jax.named_scope(f'down{g}#b={b}'):
            t0, m = GROUPS[g]
            js = range(b * BLK, (b + n) * BLK)
            for c in range(hid // CB):
                cols = slice(c * CB, (c + 1) * CB)
                for odd in range(2):
                    a = jnp.concatenate([abuf[j, s, t0:t0 + m, :] for j in js[odd::2] for s in range(4)], axis=1)
                    w = jnp.concatenate([wdb[j, :4 * CB, cols] for j in js[odd::2]], axis=0)
                    acc[odd, t0:t0 + m, cols] += jnp.dot(a, w, preferred_element_type=F32)

    def down_total(g):
        rows = pl.ds(*GROUPS[g])
        acc[0, rows, :] += acc[1, rows, :]

    def early(p):
        def step(i, carry):
            if p == 0:
                @pl.when(i == 1)
                def _():
                    x_relay(1)
            for k in range(BLK):
                gate_up(BLK * i + k, *PIECES[p])
            for k in range(BLK):
                for g in (0,) if p == 0 else (1, 2):
                    a_push(g, BLK * i + k)
            return carry
        lax.fori_loop(0, EARLY // BLK, step, 0)

    with jax.named_scope('xnear0'):
        arrived(*g_ex, 0)
        push(*g_ex, 2).start()
        x_relay(0)
    x_norm(0)
    w_start(AHEAD + EARLY)
    w_start(AHEAD + EARLY + 1)
    with jax.named_scope('gu0'):
        early(0)
    x_norm(1)
    w_start(AHEAD + EARLY + 2)
    wd_start(0)
    with jax.named_scope('gu1'):
        early(1)
    for i, first in enumerate(range(EARLY, chunks, STEP)):
        for g, b in ((0, 0), (0, 1)) if i == 0 else ((1, 0), (1, 1)):
            relay(g, b)
        wd_start(i + 1)
        with jax.named_scope('wwait'):
            for j in range(first, first + STEP):
                w_wait(j)
        with jax.named_scope('gu'):
            for j in range(first, first + STEP):
                gate_up(j, 0, nbuf.shape[0])
            for j in range(first, first + STEP):
                a_push(0, j)
    for g in (1, 2):
        for j in range(EARLY, chunks):
            a_push(g, j)
    wq_start()

    def residual(g):
        y_copy(g).wait_recv()
        t0, m = GROUPS[g]
        for t in range(t0, t0 + m, 16):
            rows = slice(t, t + 16)
            v = (xbuf[row, rows, :].astype(F32) + (acc[0, rows, :] + ybuf[rows, :])).astype(BF16)
            xpbuf[row, rows, :] = v
            xo[rows, :] = v
        push(*p_ex(g), 0).start()
        push(*p_ex(g), 1).start()
        if g == 2:
            push(*p_ex(g), 2, True).start()

    def residual_relay(g):
        arrived(*p_ex(g), 0)
        push(*p_ex(g), 2).start()

    def qkv(groups):
        for g in groups:
            arrived(*p_ex(g), 1)
            arrived(*p_ex(g), 2)
            normalise(xpbuf, 1, *GROUPS[g])
        t0 = GROUPS[groups[0]][0]
        m = sum(GROUPS[g][1] for g in groups)

        def step(i, carry):
            n = nbuf[t0:t0 + m, :]
            for k in range(2):
                j = 2 * i + k
                out = jnp.dot(n, gu_part(j, 0)[...], preferred_element_type=F32)
                qo[t0:t0 + m, pl.ds(pl.multiple_of(j * CB, CB), CB)] = out.astype(BF16)
            return carry
        lax.fori_loop(0, q_slabs // 2, step, 0)

    def finish(g):
        down_total(g)
        y_copy(g).start()

    relay(0, 2)
    relay(2, 0)
    relay(2, 1)
    down(0, 0, 2)
    relay(0, 3)
    down(1, 0, 2)
    relay(0, 4)
    down(2, 0, 2)
    down(0, 2, 2)
    relay(0, 5)
    relay(1, 2)
    down(0, 4, 2)
    finish(0)
    relay(1, 3)
    relay(1, 4)
    down(1, 2, 2)
    relay(1, 5)
    relay(2, 2)
    down(1, 4, 2)
    finish(1)
    relay(2, 3)
    relay(2, 4)
    down(2, 2, 2)
    relay(2, 5)
    with jax.named_scope('resid0'):
        residual(0)
    down(2, 4, 2)
    finish(2)
    with jax.named_scope('drain'):
        sent(gbuf.at[pl.ds(0, 3)], gs)
        sent(xbuf.at[pl.ds(0, 3)], xs)
        sent(abuf.at[:, pl.ds(0, 3)], as_)
        wq_wait()
    with jax.named_scope('resid1'):
        residual(1)
    with jax.named_scope('rrelay0'):
        residual_relay(0)
    with jax.named_scope('resid2'):
        residual(2)
    with jax.named_scope('rrelay1'):
        residual_relay(1)
    with jax.named_scope('qkv0'):
        qkv((0,))
    with jax.named_scope('xpwait'):
        arrived(*p_ex(2), 0)
    with jax.named_scope('qkv12'):
        qkv((1, 2))
    with jax.named_scope('end'):
        sent(acc.at[0], ys)
        sent(xpbuf.at[pl.ds(0, 3)], ps)


def solution(mesh):
    def per_device(residual, gain_mlp, gain_attn, w_gate, w_up, w_down, w_qkv):
        tokens, hid = residual.shape
        d_model, d_ff = w_gate.shape
        q_width = w_qkv.shape[1]
        chunks = d_ff // CB
        any_spec = pl.BlockSpec(memory_space=pl.ANY)
        vmem_spec = pl.BlockSpec(memory_space=pltpu.VMEM)
        dma = pltpu.SemaphoreType.DMA
        groups, pieces = len(GROUPS), len(PIECES)
        return pl.pallas_call(
            kernel,
            name='block',
            out_shape=(pltpu.VMEM((tokens, hid), BF16), pltpu.VMEM((tokens, q_width), BF16)),
            in_specs=[any_spec] * 7,
            out_specs=(vmem_spec, vmem_spec),
            scratch_shapes=[
                pltpu.VMEM((chunks, 2 * d_model + PAD, CB), BF16),
                pltpu.VMEM((chunks, 4 * CB + PAD, hid), BF16),
                pltpu.VMEM((chunks, 4, tokens, CB), BF16),
                pltpu.VMEM((4, tokens, hid), BF16),
                pltpu.VMEM((4, tokens, hid), BF16),
                pltpu.VMEM((tokens, d_model), BF16),
                pltpu.VMEM((2, tokens, hid), F32),
                pltpu.VMEM((tokens, hid), F32),
                pltpu.VMEM((4, 2, hid), F32),
                dma((3,)),
                dma((chunks,)),
                dma((chunks // (2 * BLK),)),
                dma,
                dma, dma((pieces, 3)),
                dma, dma((3,)),
                dma, dma((groups, chunks // BLK, 3)),
                dma, dma((groups,)),
                dma, dma((groups, 3)),
            ],
            compiler_params=pltpu.CompilerParams(collective_id=0, has_side_effects=True,
                                                 vmem_limit_bytes=66_400_000),
        )(residual, gain_mlp, gain_attn, w_gate, w_up, w_down, w_qkv)

    tok_spec, gain_spec = P('data', 'row'), P('row')
    wide_spec = P(None, ('col', 'row'))
    return jax.shard_map(
        per_device, mesh=mesh,
        in_specs=(tok_spec, gain_spec, gain_spec, wide_spec, wide_spec, P('col', 'row'), wide_spec),
        out_specs=(tok_spec, P('data', ('col', 'row'))), check_vma=False)
```

```python
import functools

import jax
import jax.numpy as jnp
from jax import lax
from jax.experimental import pallas as pl
from jax.experimental.pallas import tpu as pltpu
from jax.sharding import PartitionSpec as P

NORM_EPS = 1e-6
MESH = pl.DeviceIdType.MESH
F32 = jnp.float32
BF16 = jnp.bfloat16

CB = 256
PIECES = ((0, 64), (64, 64))
GROUPS = ((0, 64), (64, 48), (112, 16))
PAD = 16
BLK = 2
EARLY = 4
STEP = 4
AHEAD = 5


def kernel(res_h, g1_h, g2_h, wg_h, wu_h, wd_h, wq_h, xo, qo,
           wgu, wdb, abuf, xbuf, xpbuf, nbuf, acc, ybuf, gbuf,
           lsem, wsem, wdsem, wqsem, xs, xr, gs, gr, as_, ar, ys, yr, ps, pr):
    row, col = lax.axis_index('row'), lax.axis_index('col')
    mate = row + 1 - 2 * lax.rem(row, 2)
    near = lax.rem(row + 2, 4)
    far = lax.rem(mate + 2, 4)
    d_ff = wg_h.shape[1]
    chunks = d_ff // CB
    hid = res_h.shape[1]
    d_model = 4 * hid
    q_slabs = wq_h.shape[1] // CB

    def remote(src, dst, send, recv, device):
        return pltpu.make_async_remote_copy(src_ref=src, dst_ref=dst, send_sem=send, recv_sem=recv,
                                            device_id=device, device_id_type=MESH)

    def push(at, send, recv, kind, direct=False):
        slot = (row, row, row if direct else near)[kind]
        device = (near, mate, far if direct else mate)[kind]
        return remote(at(slot), at(slot), send(kind), recv(kind), {'row': device})

    def arrived(at, send, recv, kind):
        slot = (near, mate, far)[kind]
        remote(at(slot), at(slot), send(kind), recv(kind), {'row': mate}).wait_recv()

    def x_ex(p):
        t0, m = PIECES[p]
        return (lambda s: xbuf.at[s, pl.ds(t0, m)]), (lambda k: xs.at[p if p or k == 0 else 2]), (lambda k: xr.at[p, k])

    g_ex = (lambda s: gbuf.at[s]), (lambda k: gs), (lambda k: gr.at[k])

    def a_ex(g, j, b, n=1):
        t0, m = GROUPS[g]
        return (lambda s: abuf.at[pl.ds(j, n), s, pl.ds(t0, m)]), (lambda k: as_), (lambda k: ar.at[g, b, k])

    def p_ex(g):
        t0, m = GROUPS[g]
        return (lambda s: xpbuf.at[s, pl.ds(t0, m)]), (lambda k: ps), (lambda k: pr.at[g, k])

    def sent(buf, sem):
        remote(buf, buf, sem, sem, {'row': mate}).wait_send()

    def y_copy(g):
        rows = pl.ds(*GROUPS[g])
        return remote(acc.at[0, rows], ybuf.at[rows], ys, yr.at[g], {'col': 1 - col})

    def gu_part(j, half):
        return wgu.at[j, pl.ds(half * (d_model + PAD), d_model)]

    def w_start(j):
        for half, src in enumerate((wg_h, wu_h)):
            pltpu.make_async_copy(src.at[:, pl.ds(j * CB, CB)], gu_part(j, half), wsem.at[j]).start()

    def w_wait(j):
        both = wgu.at[j, pl.ds(0, 2 * d_model)]
        pltpu.make_async_copy(both, both, wsem.at[j]).wait()

    def wd_start(b):
        for j in range(b * 2 * BLK, (b + 1) * 2 * BLK):
            for s in range(4):
                pltpu.make_async_copy(wd_h.at[pl.ds(s * d_ff + j * CB, CB)], wdb.at[j, pl.ds(s * CB, CB)],
                                      wdsem.at[b]).start()

    def wd_wait(b):
        part = wdb.at[pl.ds(b * 2 * BLK, 2 * BLK), pl.ds(0, 4 * CB)]
        pltpu.make_async_copy(part, part, wdsem.at[b]).wait()

    def wq_start():
        for j in range(q_slabs):
            pltpu.make_async_copy(wq_h.at[:, pl.ds(j * CB, CB)], gu_part(j, 0), wqsem).start()

    def wq_wait():
        part = wgu.at[pl.ds(0, q_slabs), pl.ds(0, d_model)]
        pltpu.make_async_copy(part, part, wqsem).wait()

    loads = [pltpu.make_async_copy(res_h, xbuf.at[row], lsem.at[0]),
             pltpu.make_async_copy(g1_h, gbuf.at[row, 0], lsem.at[1]),
             pltpu.make_async_copy(g2_h, gbuf.at[row, 1], lsem.at[2])]
    for copy in loads:
        copy.start()
    barrier = pltpu.get_barrier_semaphore()
    for device in ({'row': mate}, {'row': near}, {'row': far}, {'col': 1 - col}):
        pl.semaphore_signal(barrier, inc=1, device_id=device, device_id_type=MESH)
    with jax.named_scope('loads'):
        for copy in loads:
            copy.wait()
    for j in range(AHEAD):
        w_start(j)
    acc[...] = jnp.zeros_like(acc)
    with jax.named_scope('barrier'):
        pl.semaphore_wait(barrier, 4)

    push(*x_ex(0), 0).start()
    push(*g_ex, 0).start()
    push(*x_ex(0), 1).start()
    push(*g_ex, 1).start()
    with jax.named_scope('xsend'):
        push(*x_ex(0), 0).wait_send()
    push(*x_ex(1), 0).start()
    push(*x_ex(1), 1).start()

    def normalise(src, which, t0, m):
        step = 16
        scales = []
        for t in range(t0, t0 + m, step):
            total = jnp.zeros((step, hid), F32)
            for q in range(4):
                v = src[q, t:t + step, :].astype(F32)
                total = total + v * v
            scales.append(lax.rsqrt(jnp.sum(total, axis=1, keepdims=True) / d_model + NORM_EPS))
        for i, t in enumerate(range(t0, t0 + m, step)):
            for q in range(4):
                v = src[q, t:t + step, :].astype(F32)
                nbuf[t:t + step, q * hid:(q + 1) * hid] = (v * scales[i] * gbuf[q, which:which + 1, :]).astype(BF16)

    with jax.named_scope('w'):
        for j in range(EARLY):
            w_wait(j)
            w_start(AHEAD + j)

    def x_relay(p):
        arrived(*x_ex(p), 0)
        push(*x_ex(p), 2).start()

    def x_norm(p):
        with jax.named_scope(f'xfar{p}'):
            for kind in (1, 2):
                if p == 0:
                    arrived(*g_ex, kind)
                arrived(*x_ex(p), kind)
        with jax.named_scope(f'norm{p}'):
            normalise(xbuf, 0, *PIECES[p])

    def gate_up(j, t0, m):
        n = nbuf[t0:t0 + m, :]
        gate = jnp.dot(n, gu_part(j, 0)[...], preferred_element_type=F32)
        up = jnp.dot(n, gu_part(j, 1)[...], preferred_element_type=F32)
        abuf[j, row, t0:t0 + m, :] = (jax.nn.silu(gate) * up).astype(BF16)

    def a_push(g, j):
        push(*a_ex(g, j, j // BLK), 0).start()
        push(*a_ex(g, j, j // BLK), 1).start()

    def relay(g, b):
        with jax.named_scope(f'relay{g}#b={b}'):
            arrived(*a_ex(g, b * BLK, b, BLK), 0)
            push(*a_ex(g, b * BLK, b, BLK), 2).start()

    def down(g, b, n=1):
        with jax.named_scope(f'dwait{g}#b={b}'):
            for i in range(b, b + n):
                arrived(*a_ex(g, i * BLK, i, BLK), 1)
                arrived(*a_ex(g, i * BLK, i, BLK), 2)
            if g == 0:
                wd_wait(b // 2)
        with jax.named_scope(f'down{g}#b={b}'):
            t0, m = GROUPS[g]
            js = range(b * BLK, (b + n) * BLK)
            for c in range(hid // CB):
                cols = slice(c * CB, (c + 1) * CB)
                for odd in range(2):
                    a = jnp.concatenate([abuf[j, s, t0:t0 + m, :] for j in js[odd::2] for s in range(4)], axis=1)
                    w = jnp.concatenate([wdb[j, :4 * CB, cols] for j in js[odd::2]], axis=0)
                    acc[odd, t0:t0 + m, cols] += jnp.dot(a, w, preferred_element_type=F32)

    def down_total(g):
        rows = pl.ds(*GROUPS[g])
        acc[0, rows, :] += acc[1, rows, :]

    def early(p):
        def step(i, carry):
            if p == 0:
                @pl.when(i == 1)
                def _():
                    x_relay(1)
            for k in range(BLK):
                gate_up(BLK * i + k, *PIECES[p])
            for k in range(BLK):
                for g in (0,) if p == 0 else (1, 2):
                    a_push(g, BLK * i + k)
            return carry
        lax.fori_loop(0, EARLY // BLK, step, 0)

    with jax.named_scope('xnear0'):
        arrived(*g_ex, 0)
        push(*g_ex, 2).start()
        x_relay(0)
    x_norm(0)
    w_start(AHEAD + EARLY)
    w_start(AHEAD + EARLY + 1)
    with jax.named_scope('gu0'):
        early(0)
    x_norm(1)
    w_start(AHEAD + EARLY + 2)
    wd_start(0)
    with jax.named_scope('gu1'):
        early(1)
    for i, first in enumerate(range(EARLY, chunks, STEP)):
        relay(0, i)
        wd_start(i + 1)
        with jax.named_scope('wwait'):
            for j in range(first, first + STEP):
                w_wait(j)
        with jax.named_scope('gu'):
            for j in range(first, first + STEP):
                gate_up(j, 0, nbuf.shape[0])
            for j in range(first, first + STEP):
                a_push(0, j)
    for g in (1, 2):
        for j in range(EARLY, chunks):
            a_push(g, j)
    wq_start()

    def residual(g):
        y_copy(g).wait_recv()
        t0, m = GROUPS[g]
        for t in range(t0, t0 + m, 16):
            rows = slice(t, t + 16)
            v = (xbuf[row, rows, :].astype(F32) + (acc[0, rows, :] + ybuf[rows, :])).astype(BF16)
            xpbuf[row, rows, :] = v
            xo[rows, :] = v
        push(*p_ex(g), 0).start()
        push(*p_ex(g), 1).start()
        if g == 2:
            push(*p_ex(g), 2, True).start()

    def residual_relay(g):
        arrived(*p_ex(g), 0)
        push(*p_ex(g), 2).start()

    def qkv(groups):
        for g in groups:
            arrived(*p_ex(g), 1)
            arrived(*p_ex(g), 2)
            normalise(xpbuf, 1, *GROUPS[g])
        t0 = GROUPS[groups[0]][0]
        m = sum(GROUPS[g][1] for g in groups)

        def step(i, carry):
            n = nbuf[t0:t0 + m, :]
            for k in range(2):
                j = 2 * i + k
                out = jnp.dot(n, gu_part(j, 0)[...], preferred_element_type=F32)
                qo[t0:t0 + m, pl.ds(pl.multiple_of(j * CB, CB), CB)] = out.astype(BF16)
            return carry
        lax.fori_loop(0, q_slabs // 2, step, 0)

    def finish(g):
        down_total(g)
        y_copy(g).start()

    for b in range(2):
        relay(1, b)
        relay(2, b)
    down(0, 0, 2)
    down(1, 0, 2)
    relay(0, 2)
    down(2, 0, 2)
    relay(0, 3)
    relay(0, 4)
    down(0, 2, 2)
    relay(0, 5)
    relay(1, 2)
    down(0, 4, 2)
    finish(0)
    relay(1, 3)
    relay(1, 4)
    down(1, 2, 2)
    relay(1, 5)
    for b in range(2, 6):
        relay(2, b)
    down(1, 4, 2)
    finish(1)
    down(2, 2, 2)
    down(2, 4, 2)
    finish(2)
    with jax.named_scope('resid0'):
        residual(0)
    with jax.named_scope('drain'):
        sent(gbuf.at[pl.ds(0, 3)], gs)
        sent(xbuf.at[pl.ds(0, 2), pl.ds(*PIECES[0])], xs.at[2])
        sent(xbuf.at[pl.ds(0, 3), pl.ds(*PIECES[1])], xs.at[1])
        sent(abuf.at[:, pl.ds(0, 3)], as_)
        wq_wait()
    with jax.named_scope('resid1'):
        residual(1)
    with jax.named_scope('rrelay0'):
        residual_relay(0)
    with jax.named_scope('resid2'):
        residual(2)
    with jax.named_scope('qkv0'):
        qkv((0,))
    with jax.named_scope('rrelay1'):
        residual_relay(1)
    with jax.named_scope('xpwait'):
        arrived(*p_ex(2), 0)
    with jax.named_scope('qkv12'):
        qkv((1, 2))
    with jax.named_scope('end'):
        sent(acc.at[0], ys)
        sent(xpbuf.at[pl.ds(0, 3)], ps)


def store_kernel(x_ref, q_ref, x_hbm, q_hbm, sem):
    copies = [pltpu.make_async_copy(x_ref, x_hbm, sem.at[0]), pltpu.make_async_copy(q_ref, q_hbm, sem.at[1])]
    for copy in copies:
        copy.start()
    for copy in copies:
        copy.wait()


def solution(mesh):
    def per_device(residual, gain_mlp, gain_attn, w_gate, w_up, w_down, w_qkv):
        tokens, hid = residual.shape
        d_model, d_ff = w_gate.shape
        q_width = w_qkv.shape[1]
        chunks = d_ff // CB
        any_spec = pl.BlockSpec(memory_space=pl.ANY)
        vmem_spec = pl.BlockSpec(memory_space=pltpu.VMEM)
        dma = pltpu.SemaphoreType.DMA
        groups, pieces = len(GROUPS), len(PIECES)
        resid_next, qkv_out = pl.pallas_call(
            kernel,
            name='block',
            out_shape=(pltpu.VMEM((tokens, hid), BF16), pltpu.VMEM((tokens, q_width), BF16)),
            in_specs=[any_spec] * 7,
            out_specs=(vmem_spec, vmem_spec),
            scratch_shapes=[
                pltpu.VMEM((chunks, 2 * d_model + PAD, CB), BF16),
                pltpu.VMEM((chunks, 4 * CB + PAD, hid), BF16),
                pltpu.VMEM((chunks, 4, tokens, CB), BF16),
                pltpu.VMEM((4, tokens, hid), BF16),
                pltpu.VMEM((4, tokens, hid), BF16),
                pltpu.VMEM((tokens, d_model), BF16),
                pltpu.VMEM((2, tokens, hid), F32),
                pltpu.VMEM((tokens, hid), F32),
                pltpu.VMEM((4, 2, hid), F32),
                dma((3,)),
                dma((chunks,)),
                dma((chunks // (2 * BLK),)),
                dma,
                dma((3,)), dma((pieces, 3)),
                dma, dma((3,)),
                dma, dma((groups, chunks // BLK, 3)),
                dma, dma((groups,)),
                dma, dma((groups, 3)),
            ],
            compiler_params=pltpu.CompilerParams(collective_id=0, has_side_effects=True,
                                                 vmem_limit_bytes=66_400_000),
        )(residual, gain_mlp, gain_attn, w_gate, w_up, w_down, w_qkv)
        return pl.pallas_call(
            store_kernel,
            name='store',
            out_shape=(jax.ShapeDtypeStruct((tokens, hid), BF16), jax.ShapeDtypeStruct((tokens, q_width), BF16)),
            in_specs=[vmem_spec, vmem_spec],
            out_specs=(any_spec, any_spec),
            scratch_shapes=[dma((2,))],
            compiler_params=pltpu.CompilerParams(vmem_limit_bytes=1 << 20),
        )(resid_next, qkv_out)

    tok_spec, gain_spec = P('data', 'row'), P('row')
    wide_spec = P(None, ('col', 'row'))
    return jax.shard_map(
        per_device, mesh=mesh,
        in_specs=(tok_spec, gain_spec, gain_spec, wide_spec, wide_spec, P('col', 'row'), wide_spec),
        out_specs=(tok_spec, P('data', ('col', 'row'))), check_vma=False)
```

```python
import functools

import jax
import jax.numpy as jnp
from jax import lax
from jax.experimental import pallas as pl
from jax.experimental.pallas import tpu as pltpu
from jax.sharding import PartitionSpec as P

NORM_EPS = 1e-6
MESH = pl.DeviceIdType.MESH
F32 = jnp.float32
BF16 = jnp.bfloat16

CB = 256
PIECES = ((0, 48), (48, 80))
GROUPS = ((0, 48), (48, 48), (96, 32))
PAD = 16
BLK = 2
EARLY = 4
STEP = 4
GRAIN = 16
DIRECT = 6
FIRST_QKV = 80
AHEAD = 5


def kernel(res_h, g1_h, g2_h, wg_h, wu_h, wd_h, wq_h, xo, qo,
           wgu, wdb, abuf, xbuf, xpbuf, nbuf, acc, ybuf, gbuf,
           lsem, wsem, wdsem, wqsem, xs, xr, gs, gr, as_, ar, ys, yr, ps, pr):
    row, col = lax.axis_index('row'), lax.axis_index('col')
    mate = row + 1 - 2 * lax.rem(row, 2)
    near = lax.rem(row + 2, 4)
    far = lax.rem(mate + 2, 4)
    d_ff = wg_h.shape[1]
    chunks = d_ff // CB
    hid = res_h.shape[1]
    d_model = 4 * hid
    q_slabs = wq_h.shape[1] // CB

    def remote(src, dst, send, recv, device):
        return pltpu.make_async_remote_copy(src_ref=src, dst_ref=dst, send_sem=send, recv_sem=recv,
                                            device_id=device, device_id_type=MESH)

    def push(at, send, recv, kind, direct=False):
        slot = (row, row, row if direct else near)[kind]
        device = (near, mate, far if direct else mate)[kind]
        return remote(at(slot), at(slot), send(kind), recv(kind), {'row': device})

    def arrived(at, send, recv, kind):
        slot = (near, mate, far)[kind]
        remote(at(slot), at(slot), send(kind), recv(kind), {'row': mate}).wait_recv()

    def x_ex(p):
        t0, m = PIECES[p]
        return (lambda s: xbuf.at[s, pl.ds(t0, m)]), (lambda k: xs.at[p if p or k == 0 else 2]), (lambda k: xr.at[p, k])

    g_ex = (lambda s: gbuf.at[s]), (lambda k: gs), (lambda k: gr.at[k])

    def a_ex(g, j, b, n=1):
        t0, m = GROUPS[g]
        return (lambda s: abuf.at[pl.ds(j, n), s, pl.ds(t0, m)]), (lambda k: as_), (lambda k: ar.at[g, b, k])

    def p_ex(i):
        return (lambda s: xpbuf.at[s, pl.ds(i * GRAIN, GRAIN)]), (lambda k: ps), (lambda k: pr.at[i, k])

    def sent(buf, sem):
        remote(buf, buf, sem, sem, {'row': mate}).wait_send()

    def y_copy(i):
        rows = pl.ds(i * GRAIN, GRAIN)
        return remote(acc.at[0, rows], ybuf.at[rows], ys, yr.at[i], {'col': 1 - col})

    def gu_part(j, half):
        return wgu.at[j, pl.ds(half * (d_model + PAD), d_model)]

    def w_start(j):
        for half, src in enumerate((wg_h, wu_h)):
            pltpu.make_async_copy(src.at[:, pl.ds(j * CB, CB)], gu_part(j, half), wsem.at[j]).start()

    def w_wait(j):
        both = wgu.at[j, pl.ds(0, 2 * d_model)]
        pltpu.make_async_copy(both, both, wsem.at[j]).wait()

    def wd_start(b):
        for j in range(b * 2 * BLK, (b + 1) * 2 * BLK):
            for s in range(4):
                pltpu.make_async_copy(wd_h.at[pl.ds(s * d_ff + j * CB, CB)], wdb.at[j, pl.ds(s * CB, CB)],
                                      wdsem.at[b]).start()

    def wd_wait(b):
        part = wdb.at[pl.ds(b * 2 * BLK, 2 * BLK), pl.ds(0, 4 * CB)]
        pltpu.make_async_copy(part, part, wdsem.at[b]).wait()

    def wq_start():
        for j in range(q_slabs):
            pltpu.make_async_copy(wq_h.at[:, pl.ds(j * CB, CB)], gu_part(j, 0), wqsem).start()

    def wq_wait():
        part = wgu.at[pl.ds(0, q_slabs), pl.ds(0, d_model)]
        pltpu.make_async_copy(part, part, wqsem).wait()

    loads = [pltpu.make_async_copy(res_h, xbuf.at[row], lsem.at[0]),
             pltpu.make_async_copy(g1_h, gbuf.at[row, 0], lsem.at[1]),
             pltpu.make_async_copy(g2_h, gbuf.at[row, 1], lsem.at[2])]
    for copy in loads:
        copy.start()
    barrier = pltpu.get_barrier_semaphore()
    for device in ({'row': mate}, {'row': near}, {'row': far}, {'col': 1 - col}):
        pl.semaphore_signal(barrier, inc=1, device_id=device, device_id_type=MESH)
    with jax.named_scope('loads'):
        for copy in loads:
            copy.wait()
    for j in range(AHEAD):
        w_start(j)
    acc[...] = jnp.zeros_like(acc)
    with jax.named_scope('barrier'):
        pl.semaphore_wait(barrier, 4)

    push(*x_ex(0), 0).start()
    push(*g_ex, 0).start()
    push(*x_ex(0), 1).start()
    push(*g_ex, 1).start()
    with jax.named_scope('xsend'):
        push(*x_ex(0), 0).wait_send()
    push(*x_ex(1), 0).start()
    push(*x_ex(1), 1).start()

    def normalise(src, which, t0, m):
        step = 16
        scales = []
        for t in range(t0, t0 + m, step):
            total = jnp.zeros((step, hid), F32)
            for q in range(4):
                v = src[q, t:t + step, :].astype(F32)
                total = total + v * v
            scales.append(lax.rsqrt(jnp.sum(total, axis=1, keepdims=True) / d_model + NORM_EPS))
        for i, t in enumerate(range(t0, t0 + m, step)):
            for q in range(4):
                v = src[q, t:t + step, :].astype(F32)
                nbuf[t:t + step, q * hid:(q + 1) * hid] = (v * scales[i] * gbuf[q, which:which + 1, :]).astype(BF16)

    def x_relay(p):
        arrived(*x_ex(p), 0)
        push(*x_ex(p), 2).start()

    def x_norm(p):
        with jax.named_scope(f'xfar{p}'):
            for kind in (1, 2):
                if p == 0:
                    arrived(*g_ex, kind)
                arrived(*x_ex(p), kind)
        with jax.named_scope(f'norm{p}'):
            normalise(xbuf, 0, *PIECES[p])

    def gate_up(j, t0, m):
        n = nbuf[t0:t0 + m, :]
        gate = jnp.dot(n, gu_part(j, 0)[...], preferred_element_type=F32)
        up = jnp.dot(n, gu_part(j, 1)[...], preferred_element_type=F32)
        abuf[j, row, t0:t0 + m, :] = (jax.nn.silu(gate) * up).astype(BF16)

    def a_push(g, j):
        push(*a_ex(g, j, j // BLK), 0).start()
        push(*a_ex(g, j, j // BLK), 1).start()

    def relay(g, b):
        with jax.named_scope(f'relay{g}#b={b}'):
            arrived(*a_ex(g, b * BLK, b, BLK), 0)
            push(*a_ex(g, b * BLK, b, BLK), 2).start()

    def down(g, b, n=1):
        with jax.named_scope(f'dwait{g}#b={b}'):
            for i in range(b, b + n):
                arrived(*a_ex(g, i * BLK, i, BLK), 1)
                arrived(*a_ex(g, i * BLK, i, BLK), 2)
            if g == 0 and b % 2 == 0:
                wd_wait(b // 2)
        with jax.named_scope(f'down{g}#b={b}'):
            t0, m = GROUPS[g]
            js = range(b * BLK, (b + n) * BLK)
            for c in range(hid // CB):
                cols = slice(c * CB, (c + 1) * CB)
                for odd in range(2):
                    a = jnp.concatenate([abuf[j, s, t0:t0 + m, :] for j in js[odd::2] for s in range(4)], axis=1)
                    w = jnp.concatenate([wdb[j, :4 * CB, cols] for j in js[odd::2]], axis=0)
                    acc[odd, t0:t0 + m, cols] += jnp.dot(a, w, preferred_element_type=F32)

    def down_total(g):
        rows = pl.ds(*GROUPS[g])
        acc[0, rows, :] += acc[1, rows, :]

    def early(p):
        def step(i, carry):
            if p == 0:
                @pl.when(i == 1)
                def _():
                    x_relay(1)
            for k in range(BLK):
                gate_up(BLK * i + k, *PIECES[p])
            for k in range(BLK):
                for g in (0,) if p == 0 else (1, 2):
                    a_push(g, BLK * i + k)
            return carry
        lax.fori_loop(0, EARLY // BLK, step, 0)

    with jax.named_scope('xnear0'):
        arrived(*g_ex, 0)
        push(*g_ex, 2).start()
        x_relay(0)
    with jax.named_scope('w'):
        for j in range(EARLY):
            w_wait(j)
            w_start(AHEAD + j)
    x_norm(0)
    w_start(AHEAD + EARLY)
    w_start(AHEAD + EARLY + 1)
    with jax.named_scope('gu0'):
        early(0)
    x_norm(1)
    w_start(AHEAD + EARLY + 2)
    with jax.named_scope('gu1'):
        early(1)
    for i, first in enumerate(range(EARLY, chunks, STEP)):
        relay(0, i)
        with jax.named_scope('wwait'):
            for j in range(first, first + STEP):
                w_wait(j)
        wd_start(i)
        with jax.named_scope('gu'):
            for j in range(first, first + STEP):
                gate_up(j, 0, nbuf.shape[0])
            for j in range(first, first + STEP):
                a_push(0, j)
    for g in (1, 2):
        for j in range(EARLY, chunks):
            a_push(g, j)
    wd_start(2)
    wq_start()

    def residual(i):
        with jax.named_scope(f'resid#i={i}'):
            y_copy(i).wait_recv()
            rows = slice(i * GRAIN, (i + 1) * GRAIN)
            v = (xbuf[row, rows, :].astype(F32) + (acc[0, rows, :] + ybuf[rows, :])).astype(BF16)
            xpbuf[row, rows, :] = v
            xo[rows, :] = v
            push(*p_ex(i), 0).start()
            push(*p_ex(i), 1).start()
            if i >= DIRECT:
                push(*p_ex(i), 2, True).start()

    def residual_relay(i):
        with jax.named_scope(f'rrelay#i={i}'):
            arrived(*p_ex(i), 0)
            if i < DIRECT:
                push(*p_ex(i), 2).start()

    def qkv(t0, m, unroll):
        with jax.named_scope(f'qwait#t={t0}'):
            for i in range(t0 // GRAIN, (t0 + m) // GRAIN):
                arrived(*p_ex(i), 1)
                arrived(*p_ex(i), 2)
        with jax.named_scope(f'qnorm#t={t0}'):
            normalise(xpbuf, 1, t0, m)

        def step(i, carry):
            n = nbuf[t0:t0 + m, :]
            for k in range(2):
                j = 2 * i + k
                out = jnp.dot(n, gu_part(j, 0)[...], preferred_element_type=F32)
                start = j * CB if isinstance(i, int) else pl.multiple_of(j * CB, CB)
                qo[t0:t0 + m, pl.ds(start, CB)] = out.astype(BF16)
            return carry
        with jax.named_scope(f'qkv#t={t0}'):
            if unroll:
                for i in range(q_slabs // 2):
                    step(i, 0)
            else:
                lax.fori_loop(0, q_slabs // 2, step, 0)

    def finish(g):
        down_total(g)
        t0, m = GROUPS[g]
        for i in range(t0 // GRAIN, (t0 + m) // GRAIN):
            y_copy(i).start()

    relay(1, 0)
    relay(2, 0)
    down(0, 0, 2)
    relay(1, 1)
    relay(2, 1)
    relay(0, 2)
    down(1, 0)
    down(2, 0)
    relay(0, 3)
    down(1, 1)
    down(0, 2)
    relay(0, 4)
    down(0, 3)
    down(2, 1)
    relay(0, 5)
    down(0, 4)
    relay(1, 2)
    down(0, 5)
    finish(0)
    relay(1, 3)
    down(1, 2)
    relay(1, 4)
    down(1, 3)
    relay(1, 5)
    down(1, 4)
    relay(2, 2)
    down(1, 5)
    finish(1)
    relay(2, 3)
    residual(0)
    down(2, 2)
    relay(2, 4)
    residual(1)
    relay(2, 5)
    down(2, 3)
    down(2, 4)
    residual(2)
    down(2, 5)
    finish(2)
    with jax.named_scope('drain'):
        sent(gbuf.at[pl.ds(0, 3)], gs)
        sent(xbuf.at[pl.ds(0, 2), pl.ds(*PIECES[0])], xs.at[2])
        sent(xbuf.at[pl.ds(0, 3), pl.ds(*PIECES[1])], xs.at[1])
        sent(abuf.at[:, pl.ds(0, 3)], as_)
        wq_wait()
    for i in range(3, 8):
        residual_relay(i - 3)
        residual(i)
    residual_relay(5)
    qkv(0, FIRST_QKV, False)
    residual_relay(6)
    residual_relay(7)
    qkv(FIRST_QKV, xo.shape[0] - FIRST_QKV, True)
    with jax.named_scope('end'):
        sent(acc.at[0], ys)
        sent(xpbuf.at[pl.ds(0, 3)], ps)


def store_kernel(x_ref, q_ref, x_hbm, q_hbm, sem):
    copies = [pltpu.make_async_copy(x_ref, x_hbm, sem.at[0]), pltpu.make_async_copy(q_ref, q_hbm, sem.at[1])]
    for copy in copies:
        copy.start()
    for copy in copies:
        copy.wait()


def solution(mesh):
    def per_device(residual, gain_mlp, gain_attn, w_gate, w_up, w_down, w_qkv):
        tokens, hid = residual.shape
        d_model, d_ff = w_gate.shape
        q_width = w_qkv.shape[1]
        chunks = d_ff // CB
        any_spec = pl.BlockSpec(memory_space=pl.ANY)
        vmem_spec = pl.BlockSpec(memory_space=pltpu.VMEM)
        dma = pltpu.SemaphoreType.DMA
        groups, pieces = len(GROUPS), len(PIECES)
        resid_next, qkv_out = pl.pallas_call(
            kernel,
            name='block',
            out_shape=(pltpu.VMEM((tokens, hid), BF16), pltpu.VMEM((tokens, q_width), BF16)),
            in_specs=[any_spec] * 7,
            out_specs=(vmem_spec, vmem_spec),
            scratch_shapes=[
                pltpu.VMEM((chunks, 2 * d_model + PAD, CB), BF16),
                pltpu.VMEM((chunks, 4 * CB + PAD, hid), BF16),
                pltpu.VMEM((chunks, 4, tokens, CB), BF16),
                pltpu.VMEM((4, tokens, hid), BF16),
                pltpu.VMEM((4, tokens, hid), BF16),
                pltpu.VMEM((tokens, d_model), BF16),
                pltpu.VMEM((2, tokens, hid), F32),
                pltpu.VMEM((tokens, hid), F32),
                pltpu.VMEM((4, 2, hid), F32),
                dma((3,)),
                dma((chunks,)),
                dma((chunks // (2 * BLK),)),
                dma,
                dma((3,)), dma((pieces, 3)),
                dma, dma((3,)),
                dma, dma((groups, chunks // BLK, 3)),
                dma, dma((tokens // GRAIN,)),
                dma, dma((tokens // GRAIN, 3)),
            ],
            compiler_params=pltpu.CompilerParams(collective_id=0, has_side_effects=True,
                                                 vmem_limit_bytes=66_400_000),
        )(residual, gain_mlp, gain_attn, w_gate, w_up, w_down, w_qkv)
        return pl.pallas_call(
            store_kernel,
            name='store',
            out_shape=(jax.ShapeDtypeStruct((tokens, hid), BF16), jax.ShapeDtypeStruct((tokens, q_width), BF16)),
            in_specs=[vmem_spec, vmem_spec],
            out_specs=(any_spec, any_spec),
            scratch_shapes=[dma((2,))],
            compiler_params=pltpu.CompilerParams(vmem_limit_bytes=1 << 20),
        )(resid_next, qkv_out)

    tok_spec, gain_spec = P('data', 'row'), P('row')
    wide_spec = P(None, ('col', 'row'))
    return jax.shard_map(
        per_device, mesh=mesh,
        in_specs=(tok_spec, gain_spec, gain_spec, wide_spec, wide_spec, P('col', 'row'), wide_spec),
        out_specs=(tok_spec, P('data', ('col', 'row'))), check_vma=False)
```

```python
import functools

import jax
import jax.numpy as jnp
from jax import lax
from jax.experimental import pallas as pl
from jax.experimental.pallas import tpu as pltpu
from jax.sharding import PartitionSpec as P

NORM_EPS = 1e-6
MESH = pl.DeviceIdType.MESH
F32 = jnp.float32
BF16 = jnp.bfloat16

CB = 256
PIECES = ((0, 48), (48, 80))
GROUPS = ((0, 48), (48, 48), (96, 32))
PAD = 16
BLK = 2
EARLY = 4
STEP = 4
GRAINS = tuple((16 * i, 16) for i in range(7)) + ((112, 8), (120, 8))
DIRECT = 7
STAGES = ((0, 64), (64, 32), (96, 32))
AHEAD = 5


def kernel(res_h, g1_h, g2_h, wg_h, wu_h, wd_h, wq_h, xo, qo,
           wgu, wdb, abuf, xbuf, xpbuf, nbuf, acc, ybuf, gbuf,
           lsem, wsem, wdsem, wqsem, xs, xr, gs, gr, as_, ar, ys, yr, ps, pr, p2):
    row, col = lax.axis_index('row'), lax.axis_index('col')
    mate = row + 1 - 2 * lax.rem(row, 2)
    near = lax.rem(mate + 2, 4)
    far = lax.rem(row + 2, 4)
    d_ff = wg_h.shape[1]
    chunks = d_ff // CB
    hid = res_h.shape[1]
    d_model = 4 * hid
    q_slabs = wq_h.shape[1] // CB

    def remote(src, dst, send, recv, device):
        return pltpu.make_async_remote_copy(src_ref=src, dst_ref=dst, send_sem=send, recv_sem=recv,
                                            device_id=device, device_id_type=MESH)

    def push(at, send, recv, kind, direct=False):
        slot = (row, row, row if direct else near)[kind]
        device = (near, mate, far if direct else mate)[kind]
        return remote(at(slot), at(slot), send(kind), recv(kind), {'row': device})

    def landed(ref, sem):
        remote(ref, ref, sem, sem, {'row': mate}).wait_recv()

    def x_ex(p):
        rows = pl.ds(*PIECES[p])
        return (lambda s: xbuf.at[s, rows]), (lambda k: xs.at[p if p or k == 0 else 2]), (lambda k: xr.at[p, min(k, 1)])

    def x_both(p):
        landed(xbuf.at[pl.ds(0, 2), pl.ds(*PIECES[p])], xr.at[p, 1])

    g_ex = (lambda s: gbuf.at[s]), (lambda k: gs), (lambda k: gr.at[min(k, 1)])

    def a_ex(g, j, b, n=1):
        rows = pl.ds(*GROUPS[g])
        return (lambda s: abuf.at[pl.ds(j, n), s, rows]), (lambda k: as_), (lambda k: ar.at[g, b, min(k, 1)])

    def a_both(g, b):
        landed(abuf.at[pl.ds(b * BLK, BLK), pl.ds(0, 2), pl.ds(*GROUPS[g])], ar.at[g, b, 1])

    def p_ex(i):
        t0, m = GRAINS[i]
        both = [t0 < first + size for first, size in STAGES].index(True)
        return (lambda s: xpbuf.at[s, pl.ds(t0, m)]), (lambda k: ps), (lambda k: p2.at[both] if k else pr.at[i])

    def near_landed(ex):
        at, _, recv = ex
        landed(at(near), recv(0))

    def sent(buf, sem):
        remote(buf, buf, sem, sem, {'row': mate}).wait_send()

    def y_copy(i):
        rows = pl.ds(*GRAINS[i])
        return remote(acc.at[0, rows], ybuf.at[rows], ys, yr.at[i], {'col': 1 - col})

    def gu_part(j, half):
        return wgu.at[j, pl.ds(half * (d_model + PAD), d_model)]

    def w_start(j):
        for half, src in enumerate((wg_h, wu_h)):
            pltpu.make_async_copy(src.at[:, pl.ds(j * CB, CB)], gu_part(j, half), wsem.at[j // EARLY]).start()

    def w_wait(q):
        part = wgu.at[pl.ds(q * EARLY, EARLY), pl.ds(0, 2 * d_model)]
        pltpu.make_async_copy(part, part, wsem.at[q]).wait()

    def wd_start(b):
        for j in range(b * 2 * BLK, (b + 1) * 2 * BLK):
            for s in range(4):
                pltpu.make_async_copy(wd_h.at[pl.ds(s * d_ff + j * CB, CB)], wdb.at[j, pl.ds(s * CB, CB)],
                                      wdsem.at[b]).start()

    def wd_wait(b):
        part = wdb.at[pl.ds(b * 2 * BLK, 2 * BLK), pl.ds(0, 4 * CB)]
        pltpu.make_async_copy(part, part, wdsem.at[b]).wait()

    def wq_start():
        for j in range(q_slabs):
            pltpu.make_async_copy(wq_h.at[:, pl.ds(j * CB, CB)], gu_part(j, 0), wqsem).start()

    def wq_wait():
        part = wgu.at[pl.ds(0, q_slabs), pl.ds(0, d_model)]
        pltpu.make_async_copy(part, part, wqsem).wait()

    loads = [pltpu.make_async_copy(res_h, xbuf.at[row], lsem.at[0]),
             pltpu.make_async_copy(g1_h, gbuf.at[row, 0], lsem.at[1]),
             pltpu.make_async_copy(g2_h, gbuf.at[row, 1], lsem.at[1])]
    for copy in loads:
        copy.start()
    barrier = pltpu.get_barrier_semaphore()
    for device in ({'row': mate}, {'row': near}, {'row': far}, {'col': 1 - col}):
        pl.semaphore_signal(barrier, inc=1, device_id=device, device_id_type=MESH)
    with jax.named_scope('loads'):
        loads[0].wait()
        pltpu.make_async_copy(gbuf.at[row], gbuf.at[row], lsem.at[1]).wait()
    for j in range(AHEAD):
        w_start(j)
    acc[...] = jnp.zeros_like(acc)
    with jax.named_scope('barrier'):
        pl.semaphore_wait(barrier, 4)

    push(*x_ex(0), 0).start()
    push(*g_ex, 0).start()
    push(*x_ex(0), 1).start()
    push(*g_ex, 1).start()
    with jax.named_scope('xsend'):
        push(*x_ex(0), 0).wait_send()
    push(*x_ex(1), 0).start()
    push(*x_ex(1), 1).start()

    def normalise(src, which, t0, m):
        step = 16
        scales = []
        for t in range(t0, t0 + m, step):
            total = jnp.zeros((step, hid), F32)
            for q in range(4):
                v = src[q, t:t + step, :].astype(F32)
                total = total + v * v
            scales.append(lax.rsqrt(jnp.sum(total, axis=1, keepdims=True) / d_model + NORM_EPS))
        for i, t in enumerate(range(t0, t0 + m, step)):
            for q in range(4):
                v = src[q, t:t + step, :].astype(F32)
                nbuf[t:t + step, q * hid:(q + 1) * hid] = (v * scales[i] * gbuf[q, which:which + 1, :]).astype(BF16)

    def x_relay(p):
        near_landed(x_ex(p))
        push(*x_ex(p), 2).start()

    def x_norm(p):
        with jax.named_scope(f'xfar{p}'):
            if p == 0:
                landed(gbuf.at[pl.ds(0, 2)], gr.at[1])
            x_both(p)
        with jax.named_scope(f'norm{p}'):
            normalise(xbuf, 0, *PIECES[p])

    def gate_up(j, t0, m):
        n = nbuf[t0:t0 + m, :]
        gate = jnp.dot(n, gu_part(j, 0)[...], preferred_element_type=F32)
        up = jnp.dot(n, gu_part(j, 1)[...], preferred_element_type=F32)
        abuf[j, row, t0:t0 + m, :] = (jax.nn.silu(gate) * up).astype(BF16)

    def a_push(g, j):
        push(*a_ex(g, j, j // BLK), 0).start()
        push(*a_ex(g, j, j // BLK), 1).start()

    def relay(g, b):
        with jax.named_scope(f'relay{g}#b={b}'):
            near_landed(a_ex(g, b * BLK, b, BLK))
            push(*a_ex(g, b * BLK, b, BLK), 2).start()

    def down(g, b, n=1):
        with jax.named_scope(f'dwait{g}#b={b}'):
            for i in range(b, b + n):
                a_both(g, i)
            if g == 0 and b % 2 == 0:
                wd_wait(b // 2)
        with jax.named_scope(f'down{g}#b={b}'):
            t0, m = GROUPS[g]
            js = range(b * BLK, (b + n) * BLK)
            for c in range(hid // CB):
                cols = slice(c * CB, (c + 1) * CB)
                for odd in range(2):
                    a = jnp.concatenate([abuf[j, s, t0:t0 + m, :] for j in js[odd::2] for s in range(4)], axis=1)
                    w = jnp.concatenate([wdb[j, :4 * CB, cols] for j in js[odd::2]], axis=0)
                    acc[odd, t0:t0 + m, cols] += jnp.dot(a, w, preferred_element_type=F32)

    def down_total(g):
        rows = pl.ds(*GROUPS[g])
        acc[0, rows, :] += acc[1, rows, :]

    def early(p):
        def step(j, carry):
            if p == 0:
                @pl.when(j == 2)
                def _():
                    x_relay(1)
            gate_up(j, *PIECES[p])
            for g in (0,) if p == 0 else (1, 2):
                a_push(g, j)
            return carry
        lax.fori_loop(0, EARLY, step, 0)

    with jax.named_scope('xnear0'):
        near_landed(g_ex)
        push(*g_ex, 2).start()
        x_relay(0)
    with jax.named_scope('w'):
        w_wait(0)
        for j in range(EARLY):
            w_start(AHEAD + j)
    x_norm(0)
    w_start(AHEAD + EARLY)
    w_start(AHEAD + EARLY + 1)
    with jax.named_scope('gu0'):
        early(0)
    x_norm(1)
    w_start(AHEAD + EARLY + 2)
    with jax.named_scope('gu1'):
        early(1)
    for i, first in enumerate(range(EARLY, chunks, STEP)):
        relay(0, i)
        with jax.named_scope('wwait'):
            w_wait(i + 1)
        wd_start(i)
        with jax.named_scope('gu'):
            for j in range(first, first + STEP):
                gate_up(j, 0, nbuf.shape[0])
            for j in range(first, first + STEP):
                a_push(0, j)
    for g in (1, 2):
        for j in range(EARLY, chunks):
            a_push(g, j)
    wd_start(2)
    wq_start()

    def residual(i):
        with jax.named_scope(f'resid#i={i}'):
            y_copy(i).wait_recv()
            rows = slice(GRAINS[i][0], sum(GRAINS[i]))
            v = (xbuf[row, rows, :].astype(F32) + (acc[0, rows, :] + ybuf[rows, :])).astype(BF16)
            xpbuf[row, rows, :] = v
            xo[rows, :] = v
            push(*p_ex(i), 0).start()
            push(*p_ex(i), 1).start()
            if i >= DIRECT:
                push(*p_ex(i), 2, True).start()

    def residual_relay(i):
        with jax.named_scope(f'rrelay#i={i}'):
            near_landed(p_ex(i))
            if i < DIRECT:
                push(*p_ex(i), 2).start()

    def next_norm(stage):
        t0, m = STAGES[stage]
        with jax.named_scope(f'qwait#s={stage}'):
            landed(xpbuf.at[pl.ds(0, 2), pl.ds(t0, m)], p2.at[stage])
        with jax.named_scope(f'qnorm#s={stage}'):
            normalise(xpbuf, 1, t0, m)

    def y_push(g):
        t0, m = GROUPS[g]
        for i, (t, _) in enumerate(GRAINS):
            if t0 <= t < t0 + m:
                y_copy(i).start()

    def y_push_on(g, core):
        @pl.when(lax.rem(row, 2) == core)
        def _():
            y_push(g)

    relay(1, 0)
    relay(2, 0)
    down(0, 0, 2)
    relay(1, 1)
    relay(2, 1)
    relay(0, 2)
    down(1, 0)
    down(2, 0)
    relay(0, 3)
    down(1, 1)
    down(0, 2)
    relay(0, 4)
    down(0, 3)
    down(2, 1)
    relay(0, 5)
    down(0, 4)
    relay(1, 2)
    down(0, 5)
    down_total(0)
    y_push(0)
    relay(1, 3)
    down(1, 2)
    relay(1, 4)
    down(1, 3)
    relay(1, 5)
    down(1, 4)
    relay(2, 2)
    down(1, 5)
    down_total(1)
    y_push_on(1, 0)
    relay(2, 3)
    residual(0)
    down(2, 2)
    y_push_on(1, 1)
    relay(2, 4)
    residual(1)
    relay(2, 5)
    down(2, 3)
    down(2, 4)
    residual(2)
    down(2, 5)
    down_total(2)
    y_push_on(2, 0)
    with jax.named_scope('drain'):
        sent(gbuf.at[pl.ds(0, 3)], gs)
        sent(xbuf.at[pl.ds(0, 2), pl.ds(*PIECES[0])], xs.at[2])
        sent(xbuf.at[pl.ds(0, 3), pl.ds(*PIECES[1])], xs.at[1])
        sent(abuf.at[:, pl.ds(0, 3)], as_)
        wq_wait()
    for i in range(3, 8):
        residual_relay(i - 3)
        residual(i)
        if i == 3:
            y_push_on(2, 1)
    residual(8)
    residual_relay(5)
    next_norm(0)
    residual_relay(6)
    next_norm(1)
    residual_relay(7)
    residual_relay(8)
    next_norm(2)
    with jax.named_scope('qkv'):
        n = nbuf[...]
        for j in range(q_slabs):
            out = jnp.dot(n, gu_part(j, 0)[...], preferred_element_type=F32)
            qo[:, j * CB:(j + 1) * CB] = out.astype(BF16)
    with jax.named_scope('end'):
        sent(acc.at[0], ys)
        sent(xpbuf.at[pl.ds(0, 3)], ps)


def store_kernel(x_ref, q_ref, x_hbm, q_hbm, sem):
    copies = [pltpu.make_async_copy(x_ref, x_hbm, sem.at[0]), pltpu.make_async_copy(q_ref, q_hbm, sem.at[1])]
    for copy in copies:
        copy.start()
    for copy in copies:
        copy.wait()


def solution(mesh):
    def per_device(residual, gain_mlp, gain_attn, w_gate, w_up, w_down, w_qkv):
        tokens, hid = residual.shape
        d_model, d_ff = w_gate.shape
        q_width = w_qkv.shape[1]
        chunks = d_ff // CB
        any_spec = pl.BlockSpec(memory_space=pl.ANY)
        vmem_spec = pl.BlockSpec(memory_space=pltpu.VMEM)
        dma = pltpu.SemaphoreType.DMA
        groups, pieces = len(GROUPS), len(PIECES)
        resid_next, qkv_out = pl.pallas_call(
            kernel,
            name='block',
            out_shape=(pltpu.VMEM((tokens, hid), BF16), pltpu.VMEM((tokens, q_width), BF16)),
            in_specs=[any_spec] * 7,
            out_specs=(vmem_spec, vmem_spec),
            scratch_shapes=[
                pltpu.VMEM((chunks, 2 * d_model + PAD, CB), BF16),
                pltpu.VMEM((chunks, 4 * CB + PAD, hid), BF16),
                pltpu.VMEM((chunks, 4, tokens, CB), BF16),
                pltpu.VMEM((4, tokens, hid), BF16),
                pltpu.VMEM((4, tokens, hid), BF16),
                pltpu.VMEM((tokens, d_model), BF16),
                pltpu.VMEM((2, tokens, hid), F32),
                pltpu.VMEM((tokens, hid), F32),
                pltpu.VMEM((4, 2, hid), F32),
                dma((2,)),
                dma((chunks // EARLY,)),
                dma((chunks // (2 * BLK),)),
                dma,
                dma((3,)), dma((pieces, 2)),
                dma, dma((2,)),
                dma, dma((groups, chunks // BLK, 2)),
                dma, dma((len(GRAINS),)),
                dma, dma((len(GRAINS),)), dma((len(STAGES),)),
            ],
            compiler_params=pltpu.CompilerParams(collective_id=0, has_side_effects=True,
                                                 vmem_limit_bytes=66_400_000),
        )(residual, gain_mlp, gain_attn, w_gate, w_up, w_down, w_qkv)
        return pl.pallas_call(
            store_kernel,
            name='store',
            out_shape=(jax.ShapeDtypeStruct((tokens, hid), BF16), jax.ShapeDtypeStruct((tokens, q_width), BF16)),
            in_specs=[vmem_spec, vmem_spec],
            out_specs=(any_spec, any_spec),
            scratch_shapes=[dma((2,))],
            compiler_params=pltpu.CompilerParams(vmem_limit_bytes=1 << 20),
        )(resid_next, qkv_out)

    tok_spec, gain_spec = P('data', 'row'), P('row')
    wide_spec = P(None, ('col', 'row'))
    return jax.shard_map(
        per_device, mesh=mesh,
        in_specs=(tok_spec, gain_spec, gain_spec, wide_spec, wide_spec, P('col', 'row'), wide_spec),
        out_specs=(tok_spec, P('data', ('col', 'row'))), check_vma=False)
```

```python
import functools

import jax
import jax.numpy as jnp
from jax import lax
from jax.experimental import pallas as pl
from jax.experimental.pallas import tpu as pltpu
from jax.sharding import PartitionSpec as P

NORM_EPS = 1e-6
MESH = pl.DeviceIdType.MESH
F32 = jnp.float32
BF16 = jnp.bfloat16

CB = 256
PIECES = ((0, 48), (48, 80))
GROUPS = ((0, 48), (48, 48), (96, 32))
PAD = 16
BLK = 2
EARLY = 4
STEP = 4
GRAINS = tuple((16 * i, 16) for i in range(7)) + ((112, 8), (120, 8))
DIRECT = 7
STAGES = ((0, 64), (64, 32), (96, 32))
AHEAD = 5


def kernel(res_h, g1_h, g2_h, wg_h, wu_h, wd_h, wq_h, xo, qo,
           wgu, wdb, abuf, xbuf, xpbuf, nbuf, acc, ybuf, gbuf,
           lsem, wsem, wdsem, wqsem, xs, xr, gs, gr, as_, ar, ys, yr, ps, pr, p2):
    row, col = lax.axis_index('row'), lax.axis_index('col')
    mate = row + 1 - 2 * lax.rem(row, 2)
    near = lax.rem(mate + 2, 4)
    far = lax.rem(row + 2, 4)
    d_ff = wg_h.shape[1]
    chunks = d_ff // CB
    hid = res_h.shape[1]
    d_model = 4 * hid
    q_slabs = wq_h.shape[1] // CB

    def remote(src, dst, send, recv, device):
        return pltpu.make_async_remote_copy(src_ref=src, dst_ref=dst, send_sem=send, recv_sem=recv,
                                            device_id=device, device_id_type=MESH)

    def push(at, send, recv, kind, direct=False):
        slot = (row, row, row if direct else near)[kind]
        device = (near, mate, far if direct else mate)[kind]
        return remote(at(slot), at(slot), send(kind), recv(kind), {'row': device})

    def landed(ref, sem):
        remote(ref, ref, sem, sem, {'row': mate}).wait_recv()

    def x_ex(p):
        rows = pl.ds(*PIECES[p])
        return (lambda s: xbuf.at[s, rows]), (lambda k: xs.at[1 if p else (0, 3, 2)[k]]), (lambda k: xr.at[p, min(k, 1)])

    def x_both(p):
        landed(xbuf.at[pl.ds(0, 2), pl.ds(*PIECES[p])], xr.at[p, 1])

    g_ex = (lambda s: gbuf.at[s]), (lambda k: gs), (lambda k: gr.at[min(k, 1)])

    def a_ex(g, j, b, n=1):
        rows = pl.ds(*GROUPS[g])
        return (lambda s: abuf.at[pl.ds(j, n), s, rows]), (lambda k: as_), (lambda k: ar.at[g, b, min(k, 1)])

    def a_both(g, b):
        landed(abuf.at[pl.ds(b * BLK, BLK), pl.ds(0, 2), pl.ds(*GROUPS[g])], ar.at[g, b, 1])

    def p_ex(i):
        t0, m = GRAINS[i]
        both = [t0 < first + size for first, size in STAGES].index(True)
        return (lambda s: xpbuf.at[s, pl.ds(t0, m)]), (lambda k: ps), (lambda k: p2.at[both] if k else pr.at[i])

    def near_landed(ex):
        at, _, recv = ex
        landed(at(near), recv(0))

    def sent(buf, sem):
        remote(buf, buf, sem, sem, {'row': mate}).wait_send()

    def y_copy(i):
        rows = pl.ds(*GRAINS[i])
        return remote(acc.at[0, rows], ybuf.at[rows], ys, yr.at[i], {'col': 1 - col})

    def gu_part(j, half):
        return wgu.at[j, pl.ds(half * (d_model + PAD), d_model)]

    def w_start(j):
        for half, src in enumerate((wg_h, wu_h)):
            pltpu.make_async_copy(src.at[:, pl.ds(j * CB, CB)], gu_part(j, half), wsem.at[j // EARLY]).start()

    def w_wait(q):
        part = wgu.at[pl.ds(q * EARLY, EARLY), pl.ds(0, 2 * d_model)]
        pltpu.make_async_copy(part, part, wsem.at[q]).wait()

    def wd_start(b):
        for j in range(b * 2 * BLK, (b + 1) * 2 * BLK):
            for s in range(4):
                pltpu.make_async_copy(wd_h.at[pl.ds(s * d_ff + j * CB, CB)], wdb.at[j, pl.ds(s * CB, CB)],
                                      wdsem.at[b]).start()

    def wd_wait(b):
        part = wdb.at[pl.ds(b * 2 * BLK, 2 * BLK), pl.ds(0, 4 * CB)]
        pltpu.make_async_copy(part, part, wdsem.at[b]).wait()

    def wq_start():
        for j in range(q_slabs):
            pltpu.make_async_copy(wq_h.at[:, pl.ds(j * CB, CB)], gu_part(j, 0), wqsem).start()

    def wq_wait():
        part = wgu.at[pl.ds(0, q_slabs), pl.ds(0, d_model)]
        pltpu.make_async_copy(part, part, wqsem).wait()

    loads = [pltpu.make_async_copy(res_h, xbuf.at[row], lsem.at[0]),
             pltpu.make_async_copy(g1_h, gbuf.at[row, 0], lsem.at[1]),
             pltpu.make_async_copy(g2_h, gbuf.at[row, 1], lsem.at[1])]
    for copy in loads:
        copy.start()
    barrier = pltpu.get_barrier_semaphore()
    for device in ({'row': mate}, {'row': near}, {'row': far}, {'col': 1 - col}):
        pl.semaphore_signal(barrier, inc=1, device_id=device, device_id_type=MESH)
    with jax.named_scope('loads'):
        loads[0].wait()
        pltpu.make_async_copy(gbuf.at[row], gbuf.at[row], lsem.at[1]).wait()
    for j in range(AHEAD):
        w_start(j)
    acc[...] = jnp.zeros_like(acc)
    with jax.named_scope('barrier'):
        pl.semaphore_wait(barrier, 4)

    @pl.when(lax.rem(row, 2) == 0)
    def _():
        push(*x_ex(0), 0).start()
        push(*x_ex(0), 1).start()

    @pl.when(lax.rem(row, 2) == 1)
    def _():
        push(*x_ex(0), 1).start()
        push(*x_ex(0), 1).wait_send()
        push(*x_ex(0), 0).start()

    push(*g_ex, 0).start()
    push(*g_ex, 1).start()
    with jax.named_scope('xsend'):
        push(*x_ex(0), 0).wait_send()
    push(*x_ex(1), 0).start()
    push(*x_ex(1), 1).start()

    def normalise(src, which, t0, m):
        step = 16
        scales = []
        for t in range(t0, t0 + m, step):
            total = jnp.zeros((step, hid), F32)
            for q in range(4):
                v = src[q, t:t + step, :].astype(F32)
                total = total + v * v
            scales.append(lax.rsqrt(jnp.sum(total, axis=1, keepdims=True) / d_model + NORM_EPS))
        for i, t in enumerate(range(t0, t0 + m, step)):
            for q in range(4):
                v = src[q, t:t + step, :].astype(F32)
                nbuf[t:t + step, q * hid:(q + 1) * hid] = (v * scales[i] * gbuf[q, which:which + 1, :]).astype(BF16)

    def x_relay(p):
        near_landed(x_ex(p))
        push(*x_ex(p), 2).start()

    def x_norm(p):
        with jax.named_scope(f'xfar{p}'):
            if p == 0:
                landed(gbuf.at[pl.ds(0, 2)], gr.at[1])
            x_both(p)
        with jax.named_scope(f'norm{p}'):
            normalise(xbuf, 0, *PIECES[p])

    def gate_up(j, t0, m):
        n = nbuf[t0:t0 + m, :]
        gate = jnp.dot(n, gu_part(j, 0)[...], preferred_element_type=F32)
        up = jnp.dot(n, gu_part(j, 1)[...], preferred_element_type=F32)
        abuf[j, row, t0:t0 + m, :] = (jax.nn.silu(gate) * up).astype(BF16)

    def a_push(g, j):
        push(*a_ex(g, j, j // BLK), 0).start()
        push(*a_ex(g, j, j // BLK), 1).start()

    def relay(g, b):
        with jax.named_scope(f'relay{g}#b={b}'):
            near_landed(a_ex(g, b * BLK, b, BLK))
            push(*a_ex(g, b * BLK, b, BLK), 2).start()

    def down(g, b, n=1):
        with jax.named_scope(f'dwait{g}#b={b}'):
            for i in range(b, b + n):
                a_both(g, i)
            if g == 0 and b % 2 == 0:
                wd_wait(b // 2)
        with jax.named_scope(f'down{g}#b={b}'):
            t0, m = GROUPS[g]
            js = range(b * BLK, (b + n) * BLK)
            for c in range(hid // CB):
                cols = slice(c * CB, (c + 1) * CB)
                for odd in range(2):
                    a = jnp.concatenate([abuf[j, s, t0:t0 + m, :] for j in js[odd::2] for s in range(4)], axis=1)
                    w = jnp.concatenate([wdb[j, :4 * CB, cols] for j in js[odd::2]], axis=0)
                    acc[odd, t0:t0 + m, cols] += jnp.dot(a, w, preferred_element_type=F32)

    def down_total(g):
        rows = pl.ds(*GROUPS[g])
        acc[0, rows, :] += acc[1, rows, :]

    def early(p):
        def step(j, carry):
            if p == 0:
                @pl.when(j == 2)
                def _():
                    x_relay(1)
            gate_up(j, *PIECES[p])
            for g in (0,) if p == 0 else (1, 2):
                a_push(g, j)
            return carry
        lax.fori_loop(0, EARLY, step, 0)

    with jax.named_scope('xnear0'):
        near_landed(g_ex)
        push(*g_ex, 2).start()
        x_relay(0)
    with jax.named_scope('w'):
        w_wait(0)
        for j in range(EARLY):
            w_start(AHEAD + j)
    x_norm(0)
    w_start(AHEAD + EARLY)
    w_start(AHEAD + EARLY + 1)
    with jax.named_scope('gu0'):
        early(0)
    x_norm(1)
    w_start(AHEAD + EARLY + 2)
    with jax.named_scope('gu1'):
        early(1)
    for i, first in enumerate(range(EARLY, chunks, STEP)):
        relay(0, i)
        with jax.named_scope('wwait'):
            w_wait(i + 1)
        wd_start(i)
        with jax.named_scope('gu'):
            for j in range(first, first + STEP):
                gate_up(j, 0, nbuf.shape[0])
            for j in range(first, first + STEP):
                a_push(0, j)
    for g in (1, 2):
        for j in range(EARLY, chunks):
            a_push(g, j)
    wd_start(2)
    wq_start()

    def residual(i):
        with jax.named_scope(f'resid#i={i}'):
            y_copy(i).wait_recv()
            rows = slice(GRAINS[i][0], sum(GRAINS[i]))
            v = (xbuf[row, rows, :].astype(F32) + (acc[0, rows, :] + ybuf[rows, :])).astype(BF16)
            xpbuf[row, rows, :] = v
            xo[rows, :] = v
            push(*p_ex(i), 0).start()
            push(*p_ex(i), 1).start()
            if i >= DIRECT:
                push(*p_ex(i), 2, True).start()

    def residual_relay(i):
        with jax.named_scope(f'rrelay#i={i}'):
            near_landed(p_ex(i))
            if i < DIRECT:
                push(*p_ex(i), 2).start()

    def next_norm(stage):
        t0, m = STAGES[stage]
        with jax.named_scope(f'qwait#s={stage}'):
            landed(xpbuf.at[pl.ds(0, 2), pl.ds(t0, m)], p2.at[stage])
        with jax.named_scope(f'qnorm#s={stage}'):
            normalise(xpbuf, 1, t0, m)

    def finish(g):
        down_total(g)
        t0, m = GROUPS[g]
        for i, (t, _) in enumerate(GRAINS):
            if t0 <= t < t0 + m:
                y_copy(i).start()

    relay(1, 0)
    relay(2, 0)
    down(0, 0, 2)
    relay(1, 1)
    relay(2, 1)
    relay(0, 2)
    down(1, 0)
    down(2, 0)
    relay(0, 3)
    down(1, 1)
    down(0, 2)
    relay(0, 4)
    down(0, 3)
    down(2, 1)
    relay(0, 5)
    down(0, 4)
    relay(1, 2)
    down(0, 5)
    finish(0)
    relay(1, 3)
    down(1, 2)
    relay(1, 4)
    down(1, 3)
    relay(1, 5)
    down(1, 4)
    relay(2, 2)
    down(1, 5)
    finish(1)
    relay(2, 3)
    residual(0)
    down(2, 2)
    relay(2, 4)
    residual(1)
    relay(2, 5)
    down(2, 3)
    down(2, 4)
    residual(2)
    down(2, 5)
    finish(2)
    with jax.named_scope('drain'):
        sent(gbuf.at[pl.ds(0, 3)], gs)
        sent(xbuf.at[0, pl.ds(*PIECES[0])], xs.at[2])

        @pl.when(lax.rem(row, 2) == 0)
        def _():
            push(*x_ex(0), 1).wait_send()
        sent(xbuf.at[pl.ds(0, 3), pl.ds(*PIECES[1])], xs.at[1])
        sent(abuf.at[:, pl.ds(0, 3)], as_)
        wq_wait()
    for i in range(3, 8):
        residual_relay(i - 3)
        residual(i)
    residual(8)
    residual_relay(5)
    next_norm(0)
    residual_relay(6)
    next_norm(1)
    residual_relay(7)
    residual_relay(8)
    next_norm(2)
    with jax.named_scope('qkv'):
        n = nbuf[...]
        for j in range(q_slabs):
            out = jnp.dot(n, gu_part(j, 0)[...], preferred_element_type=F32)
            qo[:, j * CB:(j + 1) * CB] = out.astype(BF16)
    with jax.named_scope('end'):
        sent(acc.at[0], ys)
        sent(xpbuf.at[pl.ds(0, 3)], ps)


def store_kernel(x_ref, q_ref, x_hbm, q_hbm, sem):
    copies = [pltpu.make_async_copy(x_ref, x_hbm, sem.at[0]), pltpu.make_async_copy(q_ref, q_hbm, sem.at[1])]
    for copy in copies:
        copy.start()
    for copy in copies:
        copy.wait()


def solution(mesh):
    def per_device(residual, gain_mlp, gain_attn, w_gate, w_up, w_down, w_qkv):
        tokens, hid = residual.shape
        d_model, d_ff = w_gate.shape
        q_width = w_qkv.shape[1]
        chunks = d_ff // CB
        any_spec = pl.BlockSpec(memory_space=pl.ANY)
        vmem_spec = pl.BlockSpec(memory_space=pltpu.VMEM)
        dma = pltpu.SemaphoreType.DMA
        groups, pieces = len(GROUPS), len(PIECES)
        resid_next, qkv_out = pl.pallas_call(
            kernel,
            name='block',
            out_shape=(pltpu.VMEM((tokens, hid), BF16), pltpu.VMEM((tokens, q_width), BF16)),
            in_specs=[any_spec] * 7,
            out_specs=(vmem_spec, vmem_spec),
            scratch_shapes=[
                pltpu.VMEM((chunks, 2 * d_model + PAD, CB), BF16),
                pltpu.VMEM((chunks, 4 * CB + PAD, hid), BF16),
                pltpu.VMEM((chunks, 4, tokens, CB), BF16),
                pltpu.VMEM((4, tokens, hid), BF16),
                pltpu.VMEM((4, tokens, hid), BF16),
                pltpu.VMEM((tokens, d_model), BF16),
                pltpu.VMEM((2, tokens, hid), F32),
                pltpu.VMEM((tokens, hid), F32),
                pltpu.VMEM((4, 2, hid), F32),
                dma((2,)),
                dma((chunks // EARLY,)),
                dma((chunks // (2 * BLK),)),
                dma,
                dma((4,)), dma((pieces, 2)),
                dma, dma((2,)),
                dma, dma((groups, chunks // BLK, 2)),
                dma, dma((len(GRAINS),)),
                dma, dma((len(GRAINS),)), dma((len(STAGES),)),
            ],
            compiler_params=pltpu.CompilerParams(collective_id=0, has_side_effects=True,
                                                 vmem_limit_bytes=66_400_000),
        )(residual, gain_mlp, gain_attn, w_gate, w_up, w_down, w_qkv)
        return pl.pallas_call(
            store_kernel,
            name='store',
            out_shape=(jax.ShapeDtypeStruct((tokens, hid), BF16), jax.ShapeDtypeStruct((tokens, q_width), BF16)),
            in_specs=[vmem_spec, vmem_spec],
            out_specs=(any_spec, any_spec),
            scratch_shapes=[dma((2,))],
            compiler_params=pltpu.CompilerParams(vmem_limit_bytes=1 << 20),
        )(resid_next, qkv_out)

    tok_spec, gain_spec = P('data', 'row'), P('row')
    wide_spec = P(None, ('col', 'row'))
    return jax.shard_map(
        per_device, mesh=mesh,
        in_specs=(tok_spec, gain_spec, gain_spec, wide_spec, wide_spec, P('col', 'row'), wide_spec),
        out_specs=(tok_spec, P('data', ('col', 'row'))), check_vma=False)
```
